32 devices in a mesh: mrow: 2 (over y), pcol: 16 (over z, x, core).
Axes of the slice: x: 2, y: 2, z: 4, core: 2. Of those that a mesh axis runs over, the one named last changes fastest.
Arguments:
- snapshots: bfloat16 [7424, 4096], P('mrow', 'pcol'), may hold values from -16 to 16
- area_weight: float32 [4096], P('pcol'), may hold values from 0.2 to 1
Outputs:
- gram_tiles: float32 [2, 16, 1722368], P('mrow', 'pcol')
The draws below stay inside these ranges and needn't reach their ends.
All inputs are finite; a program needn't handle non-finite values.
Results may differ from the reference program's by a relative error of at most 0.0003.
Values may be sent and summed in bfloat16 or wider, within the bound.
A program may use at most 128 MiB of HBM per device.

```python
import math
import jax
import jax.numpy as jnp
from jax import lax

MEMBERS = 7424
POINTS = 4096
N_MROW = 2
N_PCOL = 16


def draw_snapshots(key, part):
    base = jax.random.fold_in(key, 11)
    keys = jax.random.split(base, 6)
    mode_count = 96
    climate = 2.0 * jax.random.normal(keys[0], (1, POINTS), jnp.float32)
    ranks = jnp.arange(1, mode_count + 1).astype(jnp.float32)
    coeff = jax.random.normal(keys[1], (MEMBERS, mode_count), jnp.float32) * (ranks ** (-0.5))[None, :]
    freq = jax.random.randint(keys[2], (mode_count, 1), 1, 33).astype(jnp.float32)
    phase = jax.random.uniform(keys[3], (mode_count, 1), jnp.float32, 0.0, 2.0 * math.pi)
    position = (jnp.arange(POINTS).astype(jnp.float32) / POINTS)[None, :]
    shapes = math.sqrt(2.0) * jnp.cos(2.0 * math.pi * freq * position + phase)
    rough = jax.random.uniform(keys[4], (1, POINTS), jnp.float32, 0.6, 1.4)
    total_var = jnp.sum(1.0 / ranks)
    signal = jnp.dot(coeff, shapes, precision=lax.Precision.HIGHEST) / jnp.sqrt(total_var) * rough
    noise = jax.random.normal(keys[5], (MEMBERS, POINTS), jnp.float32)
    field = signal + 0.2 * noise
    return jnp.clip(climate + field, -16.0, 16.0).astype(jnp.bfloat16)


def levels(own_key, shape, cuts, low, top_value):
    loudness = 1.0
    for dim, shards_of in cuts:
        draws = jax.random.uniform(jax.random.fold_in(jax.random.fold_in(own_key, 6), dim), (shards_of,), jnp.float32, low / len(cuts), top_value / len(cuts))
        loudness = loudness * jnp.repeat(jnp.exp(draws), shape[dim] // shards_of).reshape((-1,) + (1,) * (len(shape) - 1 - dim))
    return loudness


def setup_inputs(seed: int = 0) -> dict:
    key_list = jax.random.split(jax.random.key(seed), 3)
    snapshots = draw_snapshots(jax.random.fold_in(key_list[2], 71), 0)
    area_weight = jnp.clip(jnp.exp(math.log(1.0) - 1.609438 * jax.random.uniform(key_list[1], (POINTS,), jnp.float32) ** levels(key_list[1], (POINTS,), ((0, 16),), -0.2, 0.2)), 0.2, 1.0)
    return {"snapshots": snapshots, "area_weight": area_weight}


def reference(snapshots, area_weight):
    ens_mean = lax.optimization_barrier(jnp.sum(snapshots.astype(jnp.float32), axis=0)) / MEMBERS
    anomaly = ((snapshots.astype(jnp.float32) - ens_mean[None, :]) * jnp.sqrt(area_weight)[None, :]).astype(jnp.bfloat16)
    wide = anomaly.astype(jnp.float32)
    gram = jnp.dot(wide, wide.T, precision=lax.Precision.HIGHEST, preferred_element_type=jnp.float32)
    gram = gram / (MEMBERS - 1)
    blocks = gram.reshape(N_MROW, MEMBERS // N_MROW, N_PCOL, MEMBERS // N_PCOL)
    blocks = jnp.transpose(blocks, (0, 2, 1, 3))
    return blocks.reshape(N_MROW, N_PCOL, MEMBERS // N_MROW * (MEMBERS // N_PCOL))
```

```python
import functools

import jax
import jax.numpy as jnp
from jax import lax
from jax.experimental import pallas as pl
from jax.experimental.pallas import tpu as pltpu
from jax.sharding import PartitionSpec as P

MEMBERS = 7424
MAX_CHUNKS = 8
MESH = pl.DeviceIdType.MESH


def trigger(n_row, n_col, chunks, size, tile, me):
    ratio = n_col // n_row
    root = me // ratio
    first = me % ratio * tile // 16 * 16
    last = first + tile + tile % 16 - 1
    up, down = last // size, chunks - 1 - first // size
    if isinstance(me, int):
        return down if 2 * root >= n_row else up
    return jnp.where(2 * root >= n_row, down, up)


def gather_gram(
    n_row, n_col, chunks, quick, tile, x_ref, weight_ref, out_ref, full, cols, sums, recv, send, col_recv, col_send,
    sum_recv, sum_send,
):
    rows, depth = x_ref.shape
    length = n_col // 4
    size = rows // chunks
    half = chunks // 2
    span = cols.shape[1]
    i = lax.axis_index("mrow")
    me = lax.axis_index("pcol")
    core = lax.rem(me, 2)
    side = lax.rem(me // 2, 2)
    line = me // 4
    ratio = n_col // n_row
    root = me // ratio
    offset = lax.rem(me, ratio) * tile
    aligned = pl.multiple_of(offset // 16 * 16, 16)
    my_chunk = trigger(n_row, n_col, chunks, size, tile, me)
    backward = 2 * i >= n_row

    def index(where, which, own):
        return (where * 2 + which) * 2 + own

    up, down = index(line + 1, side, core), index(line - 1, side, core)
    across, sibling = index(line, 1 - side, core), index(line, side, 1 - core)
    has_up, has_down = line + 1 < length, line >= 1
    peers = [lax.rem(i + step, n_row) for step in range(1, n_row)]
    owns_cols = root == i

    def is_end(place):
        return jnp.logical_or(place == 0, place == length - 1)

    def first_by_line(place, sign):
        if not quick:
            return jnp.int32(chunks)
        return jnp.where(is_end(place), half, jnp.where(is_end(place + sign), 0, chunks))

    end = is_end(line) if quick else line < 0

    barrier = pltpu.get_barrier_semaphore()

    def greet(row, col):
        pl.semaphore_signal(barrier, inc=1, device_id=(row, col), device_id_type=MESH)

    pl.when(has_up)(lambda: greet(i, up))
    pl.when(has_down)(lambda: greet(i, down))
    greet(i, across)
    greet(i, sibling)
    for peer in peers:
        greet(peer, me)

    def add_up(k, total):
        block = x_ref[pl.ds(pl.multiple_of(k * size, 16), size), :].astype(jnp.float32)
        return total + jnp.sum(block.reshape(size // 8, 8, depth), axis=0)

    sums[i] = lax.fori_loop(0, chunks, add_up, jnp.zeros((8, depth), jnp.float32))
    pl.semaphore_wait(barrier, 2 + len(peers) + has_up.astype(jnp.int32) + has_down.astype(jnp.int32))

    def rows_of(k):
        at = jnp.where(backward, chunks - 1 - k, k)
        return pl.ds(pl.multiple_of(at * size, 16), size)

    def part(s, k):
        return full.at[s, rows_of(k)]

    def copy(s, k, way, target):
        return pltpu.make_async_remote_copy(
            src_ref=part(s, k), dst_ref=part(s, k), send_sem=send.at[way, s], recv_sem=recv.at[s, k],
            device_id=(i, target), device_id_type=MESH,
        )

    def col_copy(s, n):
        return pltpu.make_async_remote_copy(
            src_ref=full.at[s, pl.ds(aligned, span)], dst_ref=cols.at[s], send_sem=col_send.at[n],
            recv_sem=col_recv.at[s], device_id=(peers[n], me), device_id_type=MESH,
        )

    def arrived(s, k):
        pltpu.make_async_copy(part(s, k), part(s, k), recv.at[s, k]).wait()

    def share(s, k):
        copy(s, k, 3, sibling).start()

    def to_peers(s, k):
        @pl.when(jnp.logical_and(owns_cols, k == my_chunk))
        def _():
            for n in range(len(peers)):
                col_copy(s, n).start()

    def go_up(s, k):
        pl.when(has_up)(lambda: copy(s, k, 0, up).start())

    def go_down(s, k):
        pl.when(has_down)(lambda: copy(s, k, 1, down).start())

    def sum_copy(n):
        return pltpu.make_async_remote_copy(
            src_ref=sums.at[i], dst_ref=sums.at[i], send_sem=sum_send.at[n], recv_sem=sum_recv.at[i],
            device_id=(peers[n], me), device_id_type=MESH,
        )

    for n in range(len(peers)):
        sum_copy(n).start()
    out_ref[...] = jnp.zeros_like(out_ref)
    for peer in peers:
        pltpu.make_async_copy(sums.at[peer], sums.at[peer], sum_recv.at[peer]).wait()
    mean = jnp.sum(jnp.sum(sums[...], axis=0), axis=0, keepdims=True) / MEMBERS
    root_weight = jnp.sqrt(weight_ref[...])

    def center(k):
        row = rows_of(k)
        full[me, row, :] = ((x_ref[row, :].astype(jnp.float32) - mean) * root_weight).astype(jnp.bfloat16)

    def own(k, _):
        pl.when(k + 1 < chunks)(lambda: center(k + 1))
        copy(me, k, 2, across).start()
        go_up(me, k)
        go_down(me, k)
        share(me, k)
        to_peers(me, k)
        return 0

    center(0)
    lax.fori_loop(0, chunks, own, 0)

    def valid(sign, distance):
        place = line + sign * distance
        inside = jnp.logical_and(place >= 0, place < length)
        far = distance >= 1 if sign > 0 else distance >= 0
        return jnp.logical_and(inside, far)

    def is_late(distance, k):
        return jnp.logical_and(end, jnp.logical_and(distance == 1, k >= half))

    near = jnp.where(line == 0, 1, line - 1)

    def from_sibling(t):
        d, k = t // chunks + 1, lax.rem(t, chunks)

        def take(s):
            arrived(s, k)
            to_peers(s, k)

        for sign in (-1, 1):
            pl.when(valid(sign, d))(lambda: take(index(line + sign * d, side, 1 - core)))
            pl.when(jnp.logical_and(valid(sign, d - 1), jnp.logical_not(is_late(d - 1, k))))(
                lambda: take(index(line + sign * (d - 1), 1 - side, 1 - core))
            )
        pl.when(jnp.logical_and(d == length, is_late(1, k)))(lambda: take(index(near, 1 - side, 1 - core)))

    def repeat(way, target, start):
        def one(k, _):
            copy(across, k, way, target).start()
            return 0

        lax.fori_loop(start, chunks, one, 0)

    def slot(t, _):
        d, k = t // chunks + 1, lax.rem(t, chunks)
        for sign, forward in ((-1, go_up), (1, go_down)):
            @pl.when(valid(sign, d))
            def _():
                s = index(line + sign * d, side, core)
                arrived(s, k)
                forward(s, k)
                by_line = jnp.logical_and(d == 1, k >= first_by_line(line, sign))
                pl.when(jnp.logical_not(by_line))(lambda: copy(s, k, 2, across).start())
                share(s, k)
                to_peers(s, k)

        def take(s):
            arrived(s, k)
            share(s, k)
            to_peers(s, k)

        for sign in (-1, 1):
            pl.when(jnp.logical_and(valid(sign, d - 1), jnp.logical_not(is_late(d - 1, k))))(
                lambda: take(index(line + sign * (d - 1), 1 - side, core))
            )
        pl.when(jnp.logical_and(d == length, is_late(1, k)))(lambda: take(index(near, 1 - side, core)))
        pl.when(t >= 1)(lambda: from_sibling(t - 1))

        @pl.when(jnp.logical_and(k == chunks - 1, jnp.logical_and(has_up, d == jnp.maximum(line, 1))))
        def _():
            repeat(0, up, first_by_line(line + 1, -1))

        @pl.when(jnp.logical_and(k == chunks - 1, jnp.logical_and(has_down, d == jnp.maximum(length - 1 - line, 1))))
        def _():
            repeat(1, down, first_by_line(line - 1, 1))

        lax.fori_loop(done(t - 1), done(t), lambda v, _: work(v), 0)

        @pl.when(jnp.logical_and(d == length, jnp.logical_and(k > half, end)))
        def _():
            late(k - 1)

        return 0

    lag = chunks + 1
    hurry = chunks * length - max(1, chunks // 4) if quick else chunks * length

    def done(t):
        return jnp.where(t >= hurry, t + chunks, jnp.maximum(t + chunks - lag, 0))

    def take_cols(s):
        @pl.when(owns_cols)
        def _():
            cols[s] = full[s, pl.ds(aligned, span), :]

        @pl.when(jnp.logical_not(owns_cols))
        def _():
            pltpu.make_async_copy(cols.at[s], cols.at[s], col_recv.at[s]).wait()

    def add_product(s, k):
        row = rows_of(k)
        right = cols[s]
        if span != tile:
            right = jnp.where(offset == aligned, right[:tile], right[span - tile:])
        product = lax.dot_general(
            full[s, row, :], right, (((1,), (1,)), ((), ())), preferred_element_type=jnp.float32
        )
        for b in range(out_ref.shape[0]):
            width = min(128, tile - b * 128)
            out_ref[b, row, :width] += product[:, b * 128:b * 128 + width]

    def work(v):
        d, k = v // chunks, lax.rem(v, chunks)

        def one(n, _):
            sign = 1 - 2 * (n // 4)
            cross = lax.rem(n // 2, 2)
            distance = d - cross
            place = line + sign * distance
            good = jnp.logical_and(place >= 0, place < length)
            good = jnp.logical_and(good, distance >= n // 4)
            good = jnp.logical_and(good, distance >= 0)
            good = jnp.logical_and(good, jnp.logical_not(jnp.logical_and(cross == 1, is_late(distance, k))))

            @pl.when(good)
            def _():
                s = index(place, lax.rem(side + cross, 2), lax.rem(n, 2))
                pl.when(k == 0)(lambda: take_cols(s))
                add_product(s, k)

            return 0

        lax.fori_loop(0, 8, one, 0)
        return 0

    def late(k):
        def one(n, _):
            add_product(index(near, 1 - side, n), k)
            return 0

        lax.fori_loop(0, 2, one, 0)

    def ready_own(k, _):
        s = index(line, side, 1 - core)
        arrived(s, k)
        to_peers(s, k)
        return 0

    lax.fori_loop(0, chunks, ready_own, 0)
    last = chunks * length - 1
    lax.fori_loop(0, last + 1, slot, 0)
    from_sibling(last)
    lax.fori_loop(done(last), chunks * (length + 1), lambda v, _: work(v), 0)
    pl.when(end)(lambda: late(chunks - 1))

    def sent(s, way, count):
        ref = full.at[s, pl.ds(0, count * size)]
        pltpu.make_async_copy(ref, ref, send.at[way, s]).wait()

    def some_sent(s, way, count):
        pl.when(count == chunks)(lambda: sent(s, way, chunks))
        if quick:
            pl.when(count == half)(lambda: sent(s, way, half))

    def drain(place, _):
        straight, cross = index(place, side, core), index(place, 1 - side, core)
        sent(straight, 3, chunks)
        sent(cross, 3, chunks)
        beside = jnp.logical_or(place == line + 1, place == line - 1)
        sign = place - line
        some_sent(straight, 2, jnp.where(beside, first_by_line(line, sign), chunks))
        pl.when(jnp.logical_and(has_up, place <= line))(lambda: sent(straight, 0, chunks))
        pl.when(jnp.logical_and(has_down, place >= line))(lambda: sent(straight, 1, chunks))

        @pl.when(place == line)
        def _():
            pl.when(has_up)(lambda: some_sent(cross, 0, chunks - first_by_line(line + 1, -1)))
            pl.when(has_down)(lambda: some_sent(cross, 1, chunks - first_by_line(line - 1, 1)))

        return 0

    lax.fori_loop(0, length, drain, 0)

    @pl.when(owns_cols)
    def _():
        for n in range(len(peers)):
            pltpu.make_async_copy(cols, cols, col_send.at[n]).wait()

    for n in range(len(peers)):
        pltpu.make_async_copy(sums.at[i], sums.at[i], sum_send.at[n]).wait()


def flatten(tile, group, gram_ref, flat_ref):
    many = gram_ref.shape[1] // group
    wide = group * tile // 128
    scale = jnp.float32(1.0 / (MEMBERS - 1))
    for s in range(wide):
        parts = []
        at = s * 128
        while at < (s + 1) * 128:
            r, c = at // tile, at % tile
            count = min(tile - c, (s + 1) * 128 - at)
            parts.append((r, c, count, at - s * 128))
            at += count
        lane = lax.broadcasted_iota(jnp.int32, (many, 128), 1)
        value = None
        for r, c, count, to in parts:
            shift = (to - c) % 128
            here = gram_ref[c // 128, pl.ds(r, many, stride=group), :]
            here = pltpu.roll(here, shift, 1) if shift else here
            if c % 128 + count > 128:
                then = gram_ref[c // 128 + 1, pl.ds(r, many, stride=group), :]
                then = pltpu.roll(then, shift, 1) if shift else then
                here = jnp.where(lane < to + 128 - c % 128, here, then)
            value = here if value is None else jnp.where(lane < to, value, here)
        flat_ref[pl.ds(s, many, stride=wide), :] = value * scale


def local(n_row, n_col, snapshots, area_weight):
    rows, depth = snapshots.shape
    tile = rows * n_row // n_col
    units = rows // 16
    chunks = max(n for n in range(1, MAX_CHUNKS + 1) if units % n == 0)
    size = rows // chunks
    length = n_col // 4
    ends = [*range(4), *range(n_col - 4, n_col)]
    quick = length > 2 and all(trigger(n_row, n_col, chunks, size, tile, me) < chunks // 2 for me in ends)
    span = tile + tile % 16
    blocks = -(-tile // 128)
    gram = pl.pallas_call(
        functools.partial(gather_gram, n_row, n_col, chunks, quick, tile),
        out_shape=jax.ShapeDtypeStruct((blocks, rows, 128), jnp.float32),
        in_specs=[pl.BlockSpec(memory_space=pltpu.VMEM)] * 2,
        out_specs=pl.BlockSpec(memory_space=pltpu.VMEM),
        scratch_shapes=[
            pltpu.VMEM((n_col, rows, depth), jnp.bfloat16),
            pltpu.VMEM((n_col, span, depth), jnp.bfloat16),
            pltpu.VMEM((n_row, 8, depth), jnp.float32),
            pltpu.SemaphoreType.DMA((n_col, chunks)),
            pltpu.SemaphoreType.DMA((4, n_col)),
            pltpu.SemaphoreType.DMA((n_col,)),
            pltpu.SemaphoreType.DMA((max(n_row - 1, 1),)),
            pltpu.SemaphoreType.DMA((n_row,)),
            pltpu.SemaphoreType.DMA((max(n_row - 1, 1),)),
        ],
        compiler_params=pltpu.CompilerParams(
            collective_id=0, has_side_effects=True, vmem_limit_bytes=60 * 2**20
        ),
        name="gather_gram",
    )(snapshots, area_weight.reshape(1, depth))
    group = 8
    while group * tile % 128:
        group *= 2
    groups = rows // group
    block = max((n for n in range(8, 257, 8) if groups % n == 0), default=groups)
    wide = group * tile // 128
    flat = pl.pallas_call(
        functools.partial(flatten, tile, group),
        grid=(groups // block,),
        out_shape=jax.ShapeDtypeStruct((groups * wide, 128), jnp.float32),
        in_specs=[pl.BlockSpec((blocks, block * group, 128), lambda n: (0, n, 0))],
        out_specs=pl.BlockSpec((block * wide, 128), lambda n: (n, 0)),
        name="flatten",
    )(gram)
    return flat.reshape(1, 1, rows * tile)


def solution(mesh):
    placed = (P("mrow", "pcol"), P("pcol"))
    return jax.shard_map(
        functools.partial(local, mesh.shape["mrow"], mesh.shape["pcol"]),
        mesh=mesh, in_specs=placed, out_specs=P("mrow", "pcol", None), check_vma=False,
    )
```

```python
import functools

import jax
import jax.numpy as jnp
from jax import lax
from jax.experimental import pallas as pl
from jax.experimental.pallas import tpu as pltpu
from jax.sharding import PartitionSpec as P

MEMBERS = 7424
MAX_CHUNKS = 8
MESH = pl.DeviceIdType.MESH


def trigger(n_row, n_col, chunks, size, tile, me):
    ratio = n_col // n_row
    root = me // ratio
    first = me % ratio * tile // 16 * 16
    last = first + tile + tile % 16 - 1
    up, down = last // size, chunks - 1 - first // size
    if isinstance(me, int):
        return down if 2 * root >= n_row else up
    return jnp.where(2 * root >= n_row, down, up)


def gather_gram(
    n_row, n_col, chunks, quick, tile, x_ref, weight_ref, result_ref, out_ref, full, cols, sums, recv, send, col_recv, col_send,
    sum_recv, sum_send, out_sem,
):
    rows, depth = x_ref.shape
    length = n_col // 4
    size = rows // chunks
    half = chunks // 2
    span = cols.shape[1]
    i = lax.axis_index("mrow")
    me = lax.axis_index("pcol")
    core = lax.rem(me, 2)
    side = lax.rem(me // 2, 2)
    line = me // 4
    ratio = n_col // n_row
    root = me // ratio
    offset = lax.rem(me, ratio) * tile
    aligned = pl.multiple_of(offset // 16 * 16, 16)
    my_chunk = trigger(n_row, n_col, chunks, size, tile, me)
    backward = 2 * i >= n_row

    def index(where, which, own):
        return (where * 2 + which) * 2 + own

    up, down = index(line + 1, side, core), index(line - 1, side, core)
    across, sibling = index(line, 1 - side, core), index(line, side, 1 - core)
    has_up, has_down = line + 1 < length, line >= 1
    peers = [lax.rem(i + step, n_row) for step in range(1, n_row)]
    owns_cols = root == i

    def is_end(place):
        return jnp.logical_or(place == 0, place == length - 1)

    def first_by_line(place, sign):
        if not quick:
            return jnp.int32(chunks)
        return jnp.where(is_end(place), half, jnp.where(is_end(place + sign), 0, chunks))

    end = is_end(line) if quick else line < 0

    barrier = pltpu.get_barrier_semaphore()

    def greet(row, col):
        pl.semaphore_signal(barrier, inc=1, device_id=(row, col), device_id_type=MESH)

    pl.when(has_up)(lambda: greet(i, up))
    pl.when(has_down)(lambda: greet(i, down))
    greet(i, across)
    greet(i, sibling)
    for peer in peers:
        greet(peer, me)

    def add_up(k, total):
        block = x_ref[pl.ds(pl.multiple_of(k * size, 16), size), :].astype(jnp.float32)
        return total + jnp.sum(block.reshape(size // 8, 8, depth), axis=0)

    sums[i] = lax.fori_loop(0, chunks, add_up, jnp.zeros((8, depth), jnp.float32))
    pl.semaphore_wait(barrier, 2 + len(peers) + has_up.astype(jnp.int32) + has_down.astype(jnp.int32))

    def rows_of(k):
        at = jnp.where(backward, chunks - 1 - k, k)
        return pl.ds(pl.multiple_of(at * size, 16), size)

    def part(s, k):
        return full.at[s, rows_of(k)]

    def copy(s, k, way, target):
        return pltpu.make_async_remote_copy(
            src_ref=part(s, k), dst_ref=part(s, k), send_sem=send.at[way, s], recv_sem=recv.at[s, k],
            device_id=(i, target), device_id_type=MESH,
        )

    def col_copy(s, n):
        return pltpu.make_async_remote_copy(
            src_ref=full.at[s, pl.ds(aligned, span)], dst_ref=cols.at[s], send_sem=col_send.at[n],
            recv_sem=col_recv.at[s], device_id=(peers[n], me), device_id_type=MESH,
        )

    def arrived(s, k):
        pltpu.make_async_copy(part(s, k), part(s, k), recv.at[s, k]).wait()

    def share(s, k):
        copy(s, k, 3, sibling).start()

    def to_peers(s, k):
        @pl.when(jnp.logical_and(owns_cols, k == my_chunk))
        def _():
            for n in range(len(peers)):
                col_copy(s, n).start()

    def go_up(s, k):
        pl.when(has_up)(lambda: copy(s, k, 0, up).start())

    def go_down(s, k):
        pl.when(has_down)(lambda: copy(s, k, 1, down).start())

    def sum_copy(n):
        return pltpu.make_async_remote_copy(
            src_ref=sums.at[i], dst_ref=sums.at[i], send_sem=sum_send.at[n], recv_sem=sum_recv.at[i],
            device_id=(peers[n], me), device_id_type=MESH,
        )

    for n in range(len(peers)):
        sum_copy(n).start()
    out_ref[...] = jnp.zeros_like(out_ref)
    for peer in peers:
        pltpu.make_async_copy(sums.at[peer], sums.at[peer], sum_recv.at[peer]).wait()
    mean = jnp.sum(jnp.sum(sums[...], axis=0), axis=0, keepdims=True) / MEMBERS
    root_weight = jnp.sqrt(weight_ref[...])

    def center(k):
        row = rows_of(k)
        full[me, row, :] = ((x_ref[row, :].astype(jnp.float32) - mean) * root_weight).astype(jnp.bfloat16)

    def own(k, _):
        pl.when(k + 1 < chunks)(lambda: center(k + 1))
        copy(me, k, 2, across).start()
        go_up(me, k)
        go_down(me, k)
        share(me, k)
        to_peers(me, k)
        return 0

    center(0)
    lax.fori_loop(0, chunks, own, 0)

    def valid(sign, distance):
        place = line + sign * distance
        inside = jnp.logical_and(place >= 0, place < length)
        far = distance >= 1 if sign > 0 else distance >= 0
        return jnp.logical_and(inside, far)

    near = jnp.where(line == 0, 1, line - 1)
    final = chunks * (length - 1)
    slots = final + (half if quick else chunks)

    def cross_at(t):
        w = t + jnp.where(jnp.logical_and(end, t >= chunks + half), half, 0)
        return w // chunks, lax.rem(w, chunks)

    def late_at(t):
        return jnp.logical_and(end, t >= final), t - final + half

    def from_sibling(t):
        def take(s, k):
            arrived(s, k)
            to_peers(s, k)

        d, k = t // chunks + 1, lax.rem(t, chunks)
        e, m = cross_at(t)
        for sign in (-1, 1):
            pl.when(valid(sign, d))(lambda: take(index(line + sign * d, side, 1 - core), k))
            pl.when(valid(sign, e))(lambda: take(index(line + sign * e, 1 - side, 1 - core), m))
        is_late, m = late_at(t)
        pl.when(is_late)(lambda: take(index(near, 1 - side, 1 - core), m))

    def repeat(way, target, start):
        def one(k, _):
            copy(across, k, way, target).start()
            return 0

        lax.fori_loop(start, chunks, one, 0)

    def slot(t, _):
        d, k = t // chunks + 1, lax.rem(t, chunks)
        for sign, forward in ((-1, go_up), (1, go_down)):
            @pl.when(valid(sign, d))
            def _():
                s = index(line + sign * d, side, core)
                arrived(s, k)
                forward(s, k)
                by_line = jnp.logical_and(d == 1, k >= first_by_line(line, sign))
                pl.when(jnp.logical_not(by_line))(lambda: copy(s, k, 2, across).start())
                share(s, k)
                to_peers(s, k)

        def take(s, m):
            arrived(s, m)
            share(s, m)
            to_peers(s, m)

        e, m = cross_at(t)
        for sign in (-1, 1):
            pl.when(valid(sign, e))(lambda: take(index(line + sign * e, 1 - side, core), m))
        is_late, n = late_at(t)
        pl.when(is_late)(lambda: take(index(near, 1 - side, core), n))
        pl.when(t >= 1)(lambda: from_sibling(t - 1))

        @pl.when(jnp.logical_and(k == chunks - 1, jnp.logical_and(has_up, d == jnp.maximum(line, 1))))
        def _():
            repeat(0, up, first_by_line(line + 1, -1))

        @pl.when(jnp.logical_and(k == chunks - 1, jnp.logical_and(has_down, d == jnp.maximum(length - 1 - line, 1))))
        def _():
            repeat(1, down, first_by_line(line - 1, 1))

        lax.fori_loop(done(t - 1), done(t), lambda v, _: work(v), 0)

        was_late, m = late_at(t - 1)
        pl.when(was_late)(lambda: late(m))
        return 0

    def done(t):
        lag = jnp.full_like(t, chunks + 1)
        if quick:
            lag = jnp.where(t >= final - half * end.astype(jnp.int32), jnp.maximum(1, chunks - half - (t - final)), lag)
        return jnp.maximum(t + chunks + 1 - lag, 0)

    def take_cols(s):
        @pl.when(owns_cols)
        def _():
            cols[s] = full[s, pl.ds(aligned, span), :]

        @pl.when(jnp.logical_not(owns_cols))
        def _():
            pltpu.make_async_copy(cols.at[s], cols.at[s], col_recv.at[s]).wait()

    def add_product(s, k):
        row = rows_of(k)
        right = cols[s]
        if span != tile:
            right = jnp.where(offset == aligned, right[:tile], right[span - tile:])
        product = lax.dot_general(
            full[s, row, :], right, (((1,), (1,)), ((), ())), preferred_element_type=jnp.float32
        )
        for b in range(out_ref.shape[0]):
            width = min(128, tile - b * 128)
            out_ref[b, row, :width] += product[:, b * 128:b * 128 + width]

    def work(v):
        e, m = cross_at(v - chunks)

        def one(n, _):
            sign = 1 - 2 * (n // 4)
            cross = lax.rem(n // 2, 2)
            distance = jnp.where(cross == 1, e, v // chunks)
            k = jnp.where(cross == 1, m, lax.rem(v, chunks))
            place = line + sign * distance
            good = jnp.logical_and(place >= 0, place < length)
            good = jnp.logical_and(good, distance >= n // 4)
            good = jnp.logical_and(good, jnp.logical_or(cross == 0, v >= chunks))

            @pl.when(good)
            def _():
                s = index(place, lax.rem(side + cross, 2), lax.rem(n, 2))
                pl.when(k == 0)(lambda: take_cols(s))
                add_product(s, k)

            return 0

        lax.fori_loop(0, 8, one, 0)
        return 0

    def late(k):
        def one(n, _):
            add_product(index(near, 1 - side, n), k)
            return 0

        lax.fori_loop(0, 2, one, 0)

    def ready_own(k, _):
        s = index(line, side, 1 - core)
        arrived(s, k)
        to_peers(s, k)
        return 0

    lax.fori_loop(0, chunks, ready_own, 0)
    lax.fori_loop(0, slots, slot, 0)

    def out_copy(k):
        row = rows_of(k)
        return pltpu.make_async_copy(out_ref.at[:, row, :], result_ref.at[:, row, :], out_sem)

    early = chunks - 1 if quick else 0

    def leave(k, _):
        out_copy(k).start()
        return 0

    lax.fori_loop(0, early, leave, 0)
    last = jnp.int32(slots - 1)
    from_sibling(last)
    lax.fori_loop(done(last), slots + chunks, lambda v, _: work(v), 0)
    pl.when(end)(lambda: late(chunks - 1))
    lax.fori_loop(early, chunks, leave, 0)

    def sent(s, way, count):
        ref = full.at[s, pl.ds(0, count * size)]
        pltpu.make_async_copy(ref, ref, send.at[way, s]).wait()

    def some_sent(s, way, count):
        pl.when(count == chunks)(lambda: sent(s, way, chunks))
        if quick:
            pl.when(count == half)(lambda: sent(s, way, half))

    def drain(place, _):
        straight, cross = index(place, side, core), index(place, 1 - side, core)
        sent(straight, 3, chunks)
        sent(cross, 3, chunks)
        beside = jnp.logical_or(place == line + 1, place == line - 1)
        sign = place - line
        some_sent(straight, 2, jnp.where(beside, first_by_line(line, sign), chunks))
        pl.when(jnp.logical_and(has_up, place <= line))(lambda: sent(straight, 0, chunks))
        pl.when(jnp.logical_and(has_down, place >= line))(lambda: sent(straight, 1, chunks))

        @pl.when(place == line)
        def _():
            pl.when(has_up)(lambda: some_sent(cross, 0, chunks - first_by_line(line + 1, -1)))
            pl.when(has_down)(lambda: some_sent(cross, 1, chunks - first_by_line(line - 1, 1)))

        return 0

    lax.fori_loop(0, length, drain, 0)

    @pl.when(owns_cols)
    def _():
        for n in range(len(peers)):
            pltpu.make_async_copy(cols, cols, col_send.at[n]).wait()

    for n in range(len(peers)):
        pltpu.make_async_copy(sums.at[i], sums.at[i], sum_send.at[n]).wait()
    pltpu.make_async_copy(out_ref, result_ref, out_sem).wait()


def flatten(tile, group, gram_ref, flat_ref):
    many = gram_ref.shape[1] // group
    wide = group * tile // 128
    scale = jnp.float32(1.0 / (MEMBERS - 1))
    for s in range(wide):
        parts = []
        at = s * 128
        while at < (s + 1) * 128:
            r, c = at // tile, at % tile
            count = min(tile - c, (s + 1) * 128 - at)
            parts.append((r, c, count, at - s * 128))
            at += count
        lane = lax.broadcasted_iota(jnp.int32, (many, 128), 1)
        value = None
        for r, c, count, to in parts:
            shift = (to - c) % 128
            here = gram_ref[c // 128, pl.ds(r, many, stride=group), :]
            here = pltpu.roll(here, shift, 1) if shift else here
            if c % 128 + count > 128:
                then = gram_ref[c // 128 + 1, pl.ds(r, many, stride=group), :]
                then = pltpu.roll(then, shift, 1) if shift else then
                here = jnp.where(lane < to + 128 - c % 128, here, then)
            value = here if value is None else jnp.where(lane < to, value, here)
        flat_ref[pl.ds(s, many, stride=wide), :] = value * scale


def local(n_row, n_col, snapshots, area_weight):
    rows, depth = snapshots.shape
    tile = rows * n_row // n_col
    units = rows // 16
    chunks = max(n for n in range(1, MAX_CHUNKS + 1) if units % n == 0)
    size = rows // chunks
    length = n_col // 4
    ends = [*range(4), *range(n_col - 4, n_col)]
    quick = length > 2 and all(trigger(n_row, n_col, chunks, size, tile, me) < chunks // 2 for me in ends)
    span = tile + tile % 16
    blocks = -(-tile // 128)
    gram = pl.pallas_call(
        functools.partial(gather_gram, n_row, n_col, chunks, quick, tile),
        out_shape=jax.ShapeDtypeStruct((blocks, rows, 128), jnp.float32),
        in_specs=[pl.BlockSpec(memory_space=pltpu.VMEM)] * 2,
        out_specs=pl.BlockSpec(memory_space=pl.ANY),
        scratch_shapes=[
            pltpu.VMEM((blocks, rows, 128), jnp.float32),
            pltpu.VMEM((n_col, rows, depth), jnp.bfloat16),
            pltpu.VMEM((n_col, span, depth), jnp.bfloat16),
            pltpu.VMEM((n_row, 8, depth), jnp.float32),
            pltpu.SemaphoreType.DMA((n_col, chunks)),
            pltpu.SemaphoreType.DMA((4, n_col)),
            pltpu.SemaphoreType.DMA((n_col,)),
            pltpu.SemaphoreType.DMA((max(n_row - 1, 1),)),
            pltpu.SemaphoreType.DMA((n_row,)),
            pltpu.SemaphoreType.DMA((max(n_row - 1, 1),)),
            pltpu.SemaphoreType.DMA,
        ],
        compiler_params=pltpu.CompilerParams(
            collective_id=0, has_side_effects=True, vmem_limit_bytes=60 * 2**20
        ),
        name="gather_gram",
    )(snapshots, area_weight.reshape(1, depth))
    group = 8
    while group * tile % 128:
        group *= 2
    groups = rows // group
    block = max((n for n in range(8, 257, 8) if groups % n == 0), default=groups)
    wide = group * tile // 128
    flat = pl.pallas_call(
        functools.partial(flatten, tile, group),
        grid=(pl.cdiv(groups, block),),
        out_shape=jax.ShapeDtypeStruct((groups * wide, 128), jnp.float32),
        in_specs=[pl.BlockSpec((blocks, block * group, 128), lambda n: (0, n, 0))],
        out_specs=pl.BlockSpec((block * wide, 128), lambda n: (n, 0)),
        name="flatten",
    )(gram)
    return flat.reshape(1, 1, rows * tile)


def solution(mesh):
    placed = (P("mrow", "pcol"), P("pcol"))
    return jax.shard_map(
        functools.partial(local, mesh.shape["mrow"], mesh.shape["pcol"]),
        mesh=mesh, in_specs=placed, out_specs=P("mrow", "pcol", None), check_vma=False,
    )
```

```python
import functools

import jax
import jax.numpy as jnp
from jax import lax
from jax.experimental import pallas as pl
from jax.experimental.pallas import tpu as pltpu
from jax.sharding import PartitionSpec as P

MEMBERS = 7424
MAX_CHUNKS = 8
PIECES = 6
MESH = pl.DeviceIdType.MESH


def trigger(n_row, n_col, chunks, size, tile, me):
    ratio = n_col // n_row
    root = me // ratio
    first = me % ratio * tile // 16 * 16
    last = first + tile + tile % 16 - 1
    up, down = last // size, chunks - 1 - first // size
    if isinstance(me, int):
        return down if 2 * root >= n_row else up
    return jnp.where(2 * root >= n_row, down, up)


def gather_gram(
    n_row, n_col, chunks, quick, tile, x_ref, weight_ref, out_ref, full, cols, sums, recv, send, col_recv, col_send,
    sum_recv, sum_send,
):
    rows, depth = x_ref.shape
    length = n_col // 4
    size = rows // chunks
    half = chunks // 2
    span = cols.shape[1]
    i = lax.axis_index("mrow")
    me = lax.axis_index("pcol")
    core = lax.rem(me, 2)
    side = lax.rem(me // 2, 2)
    line = me // 4
    ratio = n_col // n_row
    root = me // ratio
    offset = lax.rem(me, ratio) * tile
    aligned = pl.multiple_of(offset // 16 * 16, 16)
    my_chunk = trigger(n_row, n_col, chunks, size, tile, me)
    backward = 2 * i >= n_row

    def index(where, which, own):
        return (where * 2 + which) * 2 + own

    up, down = index(line + 1, side, core), index(line - 1, side, core)
    across, sibling = index(line, 1 - side, core), index(line, side, 1 - core)
    has_up, has_down = line + 1 < length, line >= 1
    peers = [lax.rem(i + step, n_row) for step in range(1, n_row)]
    owns_cols = root == i

    def is_end(place):
        return jnp.logical_or(place == 0, place == length - 1)

    def first_by_line(place, sign):
        if not quick:
            return jnp.int32(chunks)
        return jnp.where(is_end(place), half, jnp.where(is_end(place + sign), 0, chunks))

    end = is_end(line) if quick else line < 0

    barrier = pltpu.get_barrier_semaphore()

    def greet(row, col):
        pl.semaphore_signal(barrier, inc=1, device_id=(row, col), device_id_type=MESH)

    pl.when(has_up)(lambda: greet(i, up))
    pl.when(has_down)(lambda: greet(i, down))
    greet(i, across)
    greet(i, sibling)
    for peer in peers:
        greet(peer, me)

    def add_up(k, total):
        block = x_ref[pl.ds(pl.multiple_of(k * size, 16), size), :].astype(jnp.float32)
        return total + jnp.sum(block.reshape(size // 8, 8, depth), axis=0)

    sums[i] = lax.fori_loop(0, chunks, add_up, jnp.zeros((8, depth), jnp.float32))
    pl.semaphore_wait(barrier, 2 + len(peers) + has_up.astype(jnp.int32) + has_down.astype(jnp.int32))

    def rows_of(k):
        at = jnp.where(backward, chunks - 1 - k, k)
        return pl.ds(pl.multiple_of(at * size, 16), size)

    def part(s, k):
        return full.at[s, rows_of(k)]

    def copy(s, k, way, target):
        return pltpu.make_async_remote_copy(
            src_ref=part(s, k), dst_ref=part(s, k), send_sem=send.at[way, s], recv_sem=recv.at[s, k],
            device_id=(i, target), device_id_type=MESH,
        )

    def col_copy(s, n):
        return pltpu.make_async_remote_copy(
            src_ref=full.at[s, pl.ds(aligned, span)], dst_ref=cols.at[s], send_sem=col_send.at[n],
            recv_sem=col_recv.at[s], device_id=(peers[n], me), device_id_type=MESH,
        )

    def arrived(s, k):
        pltpu.make_async_copy(part(s, k), part(s, k), recv.at[s, k]).wait()

    def share(s, k):
        copy(s, k, 3, sibling).start()

    def to_peers(s, k):
        @pl.when(jnp.logical_and(owns_cols, k == my_chunk))
        def _():
            for n in range(len(peers)):
                col_copy(s, n).start()

    def go_up(s, k):
        pl.when(has_up)(lambda: copy(s, k, 0, up).start())

    def go_down(s, k):
        pl.when(has_down)(lambda: copy(s, k, 1, down).start())

    def sum_copy(n):
        return pltpu.make_async_remote_copy(
            src_ref=sums.at[i], dst_ref=sums.at[i], send_sem=sum_send.at[n], recv_sem=sum_recv.at[i],
            device_id=(peers[n], me), device_id_type=MESH,
        )

    for n in range(len(peers)):
        sum_copy(n).start()
    out_ref[...] = jnp.zeros_like(out_ref)
    for peer in peers:
        pltpu.make_async_copy(sums.at[peer], sums.at[peer], sum_recv.at[peer]).wait()
    mean = jnp.sum(jnp.sum(sums[...], axis=0), axis=0, keepdims=True) / MEMBERS
    root_weight = jnp.sqrt(weight_ref[...])

    def center(k):
        row = rows_of(k)
        full[me, row, :] = ((x_ref[row, :].astype(jnp.float32) - mean) * root_weight).astype(jnp.bfloat16)

    def own(k, _):
        pl.when(k + 1 < chunks)(lambda: center(k + 1))
        copy(me, k, 2, across).start()
        go_up(me, k)
        go_down(me, k)
        share(me, k)
        to_peers(me, k)
        return 0

    center(0)
    lax.fori_loop(0, chunks, own, 0)

    def valid(sign, distance):
        place = line + sign * distance
        inside = jnp.logical_and(place >= 0, place < length)
        far = distance >= 1 if sign > 0 else distance >= 0
        return jnp.logical_and(inside, far)

    near = jnp.where(line == 0, 1, line - 1)
    final = chunks * (length - 1)
    slots = final + (half if quick else chunks)

    def cross_at(t):
        w = t + jnp.where(jnp.logical_and(end, t >= chunks + half), half, 0)
        return w // chunks, lax.rem(w, chunks)

    def late_at(t):
        return jnp.logical_and(end, t >= final), t - final + half

    def from_sibling(t):
        def take(s, k):
            arrived(s, k)
            to_peers(s, k)

        d, k = t // chunks + 1, lax.rem(t, chunks)
        e, m = cross_at(t)
        for sign in (-1, 1):
            pl.when(valid(sign, d))(lambda: take(index(line + sign * d, side, 1 - core), k))
            pl.when(valid(sign, e))(lambda: take(index(line + sign * e, 1 - side, 1 - core), m))
        is_late, m = late_at(t)
        pl.when(is_late)(lambda: take(index(near, 1 - side, 1 - core), m))

    def repeat(way, target, start):
        def one(k, _):
            copy(across, k, way, target).start()
            return 0

        lax.fori_loop(start, chunks, one, 0)

    def slot(t, _):
        d, k = t // chunks + 1, lax.rem(t, chunks)
        for sign, forward in ((-1, go_up), (1, go_down)):
            @pl.when(valid(sign, d))
            def _():
                s = index(line + sign * d, side, core)
                arrived(s, k)
                forward(s, k)
                by_line = jnp.logical_and(d == 1, k >= first_by_line(line, sign))
                pl.when(jnp.logical_not(by_line))(lambda: copy(s, k, 2, across).start())
                share(s, k)
                to_peers(s, k)

        def take(s, m):
            arrived(s, m)
            share(s, m)
            to_peers(s, m)

        e, m = cross_at(t)
        for sign in (-1, 1):
            pl.when(valid(sign, e))(lambda: take(index(line + sign * e, 1 - side, core), m))
        is_late, n = late_at(t)
        pl.when(is_late)(lambda: take(index(near, 1 - side, core), n))
        pl.when(t >= 1)(lambda: from_sibling(t - 1))

        @pl.when(jnp.logical_and(k == chunks - 1, jnp.logical_and(has_up, d == jnp.maximum(line, 1))))
        def _():
            repeat(0, up, first_by_line(line + 1, -1))

        @pl.when(jnp.logical_and(k == chunks - 1, jnp.logical_and(has_down, d == jnp.maximum(length - 1 - line, 1))))
        def _():
            repeat(1, down, first_by_line(line - 1, 1))

        lax.fori_loop(done(t - 1), done(t), lambda v, _: work(v), 0)

        was_late, m = late_at(t - 1)
        pl.when(was_late)(lambda: late(m))
        return 0

    def done(t):
        lag = jnp.full_like(t, chunks + 1)
        if quick:
            lag = jnp.where(t >= final - half * end.astype(jnp.int32), jnp.maximum(1, chunks - half - (t - final)), lag)
        return jnp.maximum(t + chunks + 1 - lag, 0)

    def take_cols(s):
        @pl.when(owns_cols)
        def _():
            cols[s] = full[s, pl.ds(aligned, span), :]

        @pl.when(jnp.logical_not(owns_cols))
        def _():
            pltpu.make_async_copy(cols.at[s], cols.at[s], col_recv.at[s]).wait()

    def add_product(s, k):
        row = rows_of(k)
        right = cols[s]
        if span != tile:
            right = jnp.where(offset == aligned, right[:tile], right[span - tile:])
        product = lax.dot_general(
            full[s, row, :], right, (((1,), (1,)), ((), ())), preferred_element_type=jnp.float32
        )
        for b in range(out_ref.shape[0]):
            width = min(128, tile - b * 128)
            out_ref[b, row, :width] += product[:, b * 128:b * 128 + width]

    def work(v):
        e, m = cross_at(v - chunks)

        def one(n, _):
            sign = 1 - 2 * (n // 4)
            cross = lax.rem(n // 2, 2)
            distance = jnp.where(cross == 1, e, v // chunks)
            k = jnp.where(cross == 1, m, lax.rem(v, chunks))
            place = line + sign * distance
            good = jnp.logical_and(place >= 0, place < length)
            good = jnp.logical_and(good, distance >= n // 4)
            good = jnp.logical_and(good, jnp.logical_or(cross == 0, v >= chunks))

            @pl.when(good)
            def _():
                s = index(place, lax.rem(side + cross, 2), lax.rem(n, 2))
                pl.when(k == 0)(lambda: take_cols(s))
                add_product(s, k)

            return 0

        lax.fori_loop(0, 8, one, 0)
        return 0

    def late(k):
        def one(n, _):
            add_product(index(near, 1 - side, n), k)
            return 0

        lax.fori_loop(0, 2, one, 0)

    def ready_own(k, _):
        s = index(line, side, 1 - core)
        arrived(s, k)
        to_peers(s, k)
        return 0

    lax.fori_loop(0, chunks, ready_own, 0)
    lax.fori_loop(0, slots, slot, 0)

    last = jnp.int32(slots - 1)
    from_sibling(last)
    lax.fori_loop(done(last), slots + chunks, lambda v, _: work(v), 0)
    pl.when(end)(lambda: late(chunks - 1))

    def sent(s, way, count):
        ref = full.at[s, pl.ds(0, count * size)]
        pltpu.make_async_copy(ref, ref, send.at[way, s]).wait()

    def some_sent(s, way, count):
        pl.when(count == chunks)(lambda: sent(s, way, chunks))
        if quick:
            pl.when(count == half)(lambda: sent(s, way, half))

    def drain(place, _):
        straight, cross = index(place, side, core), index(place, 1 - side, core)
        sent(straight, 3, chunks)
        sent(cross, 3, chunks)
        beside = jnp.logical_or(place == line + 1, place == line - 1)
        sign = place - line
        some_sent(straight, 2, jnp.where(beside, first_by_line(line, sign), chunks))
        pl.when(jnp.logical_and(has_up, place <= line))(lambda: sent(straight, 0, chunks))
        pl.when(jnp.logical_and(has_down, place >= line))(lambda: sent(straight, 1, chunks))

        @pl.when(place == line)
        def _():
            pl.when(has_up)(lambda: some_sent(cross, 0, chunks - first_by_line(line + 1, -1)))
            pl.when(has_down)(lambda: some_sent(cross, 1, chunks - first_by_line(line - 1, 1)))

        return 0

    lax.fori_loop(0, length, drain, 0)

    @pl.when(owns_cols)
    def _():
        for n in range(len(peers)):
            pltpu.make_async_copy(cols, cols, col_send.at[n]).wait()

    for n in range(len(peers)):
        pltpu.make_async_copy(sums.at[i], sums.at[i], sum_send.at[n]).wait()


def flatten(tile, group, block, gram_ref, flat_ref, buffer, sem):
    groups = gram_ref.shape[1] // group
    wide = group * tile // 128
    scale = jnp.float32(1.0 / (MEMBERS - 1))
    for start in range(0, groups, block):
        many = min(block, groups - start)
        lane = lax.broadcasted_iota(jnp.int32, (many, 128), 1)
        for s in range(wide):
            value = None
            at = s * 128
            while at < (s + 1) * 128:
                r, c, to = at // tile, at % tile, at - s * 128
                count = min(tile - c, (s + 1) * 128 - at)
                shift = (to - c) % 128
                row = pl.ds(start * group + r, many, stride=group)
                here = gram_ref[c // 128, row, :]
                here = pltpu.roll(here, shift, 1) if shift else here
                if c % 128 + count > 128:
                    then = gram_ref[c // 128 + 1, row, :]
                    then = pltpu.roll(then, shift, 1) if shift else then
                    here = jnp.where(lane < to + 128 - c % 128, here, then)
                value = here if value is None else jnp.where(lane < to, value, here)
                at += count
            buffer[pl.ds(start * wide + s, many, stride=wide), :] = value * scale
        piece = pl.ds(start * wide, many * wide)
        pltpu.make_async_copy(buffer.at[piece], flat_ref.at[piece], sem).start()
    pltpu.make_async_copy(buffer, flat_ref, sem).wait()


def local(n_row, n_col, snapshots, area_weight):
    rows, depth = snapshots.shape
    tile = rows * n_row // n_col
    units = rows // 16
    chunks = max(n for n in range(1, MAX_CHUNKS + 1) if units % n == 0)
    size = rows // chunks
    length = n_col // 4
    ends = [*range(4), *range(n_col - 4, n_col)]
    quick = length > 2 and all(trigger(n_row, n_col, chunks, size, tile, me) < chunks // 2 for me in ends)
    span = tile + tile % 16
    blocks = -(-tile // 128)
    gram = pl.pallas_call(
        functools.partial(gather_gram, n_row, n_col, chunks, quick, tile),
        out_shape=jax.ShapeDtypeStruct((blocks, rows, 128), jnp.float32),
        in_specs=[pl.BlockSpec(memory_space=pltpu.VMEM)] * 2,
        out_specs=pl.BlockSpec(memory_space=pltpu.VMEM),
        scratch_shapes=[
            pltpu.VMEM((n_col, rows, depth), jnp.bfloat16),
            pltpu.VMEM((n_col, span, depth), jnp.bfloat16),
            pltpu.VMEM((n_row, 8, depth), jnp.float32),
            pltpu.SemaphoreType.DMA((n_col, chunks)),
            pltpu.SemaphoreType.DMA((4, n_col)),
            pltpu.SemaphoreType.DMA((n_col,)),
            pltpu.SemaphoreType.DMA((max(n_row - 1, 1),)),
            pltpu.SemaphoreType.DMA((n_row,)),
            pltpu.SemaphoreType.DMA((max(n_row - 1, 1),)),
        ],
        compiler_params=pltpu.CompilerParams(
            collective_id=0, has_side_effects=True, vmem_limit_bytes=44 * 2**20
        ),
        name="gather_gram",
    )(snapshots, area_weight.reshape(1, depth))
    group = 8
    while group * tile % 128:
        group *= 2
    groups = rows // group
    block = (groups // PIECES + 7) // 8 * 8
    flat_shape = (groups * group * tile // 128, 128)
    flat = pl.pallas_call(
        functools.partial(flatten, tile, group, block),
        out_shape=jax.ShapeDtypeStruct(flat_shape, jnp.float32),
        in_specs=[pl.BlockSpec(memory_space=pltpu.VMEM)],
        out_specs=pl.BlockSpec(memory_space=pl.ANY),
        scratch_shapes=[pltpu.VMEM(flat_shape, jnp.float32), pltpu.SemaphoreType.DMA],
        compiler_params=pltpu.CompilerParams(vmem_limit_bytes=24 * 2**20),
        name="flatten",
    )(gram)
    return flat.reshape(1, 1, rows * tile)


def solution(mesh):
    placed = (P("mrow", "pcol"), P("pcol"))
    return jax.shard_map(
        functools.partial(local, mesh.shape["mrow"], mesh.shape["pcol"]),
        mesh=mesh, in_specs=placed, out_specs=P("mrow", "pcol", None), check_vma=False,
    )
```

```python
import functools

import jax
import jax.numpy as jnp
from jax import lax
from jax.experimental import pallas as pl
from jax.experimental.pallas import tpu as pltpu
from jax.sharding import PartitionSpec as P

MEMBERS = 7424
MAX_CHUNKS = 8
PIECES = 6
MESH = pl.DeviceIdType.MESH


def trigger(n_row, n_col, chunks, size, tile, me):
    ratio = n_col // n_row
    root = me // ratio
    first = me % ratio * tile // 16 * 16
    last = first + tile + tile % 16 - 1
    up, down = last // size, chunks - 1 - first // size
    if isinstance(me, int):
        return down if 2 * root >= n_row else up
    return jnp.where(2 * root >= n_row, down, up)


def gather_gram(
    n_row, n_col, chunks, quick, tile, x_ref, weight_ref, out_ref, full, cols, sums, recv, send, col_recv, col_send,
    sum_recv, sum_send,
):
    rows, depth = x_ref.shape
    length = n_col // 4
    size = rows // chunks
    half = chunks // 2
    span = cols.shape[1]
    i = lax.axis_index("mrow")
    me = lax.axis_index("pcol")
    core = lax.rem(me, 2)
    side = lax.rem(me // 2, 2)
    line = me // 4
    ratio = n_col // n_row
    root = me // ratio
    offset = lax.rem(me, ratio) * tile
    aligned = pl.multiple_of(offset // 16 * 16, 16)
    my_chunk = trigger(n_row, n_col, chunks, size, tile, me)
    backward = 2 * i >= n_row

    def index(where, which, own):
        return (where * 2 + which) * 2 + own

    up, down = index(line + 1, side, core), index(line - 1, side, core)
    across, sibling = index(line, 1 - side, core), index(line, side, 1 - core)
    has_up, has_down = line + 1 < length, line >= 1
    peers = [lax.rem(i + step, n_row) for step in range(1, n_row)]
    owns_cols = root == i

    def is_end(place):
        return jnp.logical_or(place == 0, place == length - 1)

    def first_by_line(place, sign):
        if not quick:
            return jnp.int32(chunks)
        return jnp.where(is_end(place), half, jnp.where(is_end(place + sign), 0, chunks))

    end = is_end(line) if quick else line < 0

    barrier = pltpu.get_barrier_semaphore()

    def greet(row, col):
        pl.semaphore_signal(barrier, inc=1, device_id=(row, col), device_id_type=MESH)

    pl.when(has_up)(lambda: greet(i, up))
    pl.when(has_down)(lambda: greet(i, down))
    greet(i, across)
    greet(i, sibling)
    for peer in peers:
        greet(peer, me)

    def add_up(k, total):
        block = x_ref[pl.ds(pl.multiple_of(k * size, 16), size), :].astype(jnp.float32)
        return total + jnp.sum(block.reshape(size // 8, 8, depth), axis=0)

    sums[i] = lax.fori_loop(0, chunks, add_up, jnp.zeros((8, depth), jnp.float32))
    pl.semaphore_wait(barrier, 2 + len(peers) + has_up.astype(jnp.int32) + has_down.astype(jnp.int32))

    def swapped(s, k):
        if not quick:
            return k
        swap = jnp.logical_and((lax.rem(s // 2, 2) == 0) != backward, k < half)
        return jnp.where(swap, lax.rem(k + half // 2, half), k)

    def rows_of(s, k):
        at = swapped(s, k)
        at = jnp.where(backward, chunks - 1 - at, at)
        return pl.ds(pl.multiple_of(at * size, 16), size)

    def part(s, k):
        return full.at[s, rows_of(s, k)]

    def copy(s, k, way, target):
        return pltpu.make_async_remote_copy(
            src_ref=part(s, k), dst_ref=part(s, k), send_sem=send.at[way, s], recv_sem=recv.at[s, k],
            device_id=(i, target), device_id_type=MESH,
        )

    def col_copy(s, n):
        return pltpu.make_async_remote_copy(
            src_ref=full.at[s, pl.ds(aligned, span)], dst_ref=cols.at[s], send_sem=col_send.at[n],
            recv_sem=col_recv.at[s], device_id=(peers[n], me), device_id_type=MESH,
        )

    def arrived(s, k):
        pltpu.make_async_copy(part(s, k), part(s, k), recv.at[s, k]).wait()

    def share(s, k):
        copy(s, k, 3, sibling).start()

    def to_peers(s, k):
        @pl.when(jnp.logical_and(owns_cols, swapped(s, k) == my_chunk))
        def _():
            for n in range(len(peers)):
                col_copy(s, n).start()

    def go_up(s, k):
        pl.when(has_up)(lambda: copy(s, k, 0, up).start())

    def go_down(s, k):
        pl.when(has_down)(lambda: copy(s, k, 1, down).start())

    def sum_copy(n):
        return pltpu.make_async_remote_copy(
            src_ref=sums.at[i], dst_ref=sums.at[i], send_sem=sum_send.at[n], recv_sem=sum_recv.at[i],
            device_id=(peers[n], me), device_id_type=MESH,
        )

    for n in range(len(peers)):
        sum_copy(n).start()
    out_ref[...] = jnp.zeros_like(out_ref)
    for peer in peers:
        pltpu.make_async_copy(sums.at[peer], sums.at[peer], sum_recv.at[peer]).wait()
    mean = jnp.sum(jnp.sum(sums[...], axis=0), axis=0, keepdims=True) / MEMBERS
    root_weight = jnp.sqrt(weight_ref[...])

    def center(k):
        row = rows_of(me, k)
        full[me, row, :] = ((x_ref[row, :].astype(jnp.float32) - mean) * root_weight).astype(jnp.bfloat16)

    def own(k, _):
        pl.when(k + 1 < chunks)(lambda: center(k + 1))
        copy(me, k, 2, across).start()
        go_up(me, k)
        go_down(me, k)
        share(me, k)
        to_peers(me, k)
        return 0

    center(0)
    lax.fori_loop(0, chunks, own, 0)

    def valid(sign, distance):
        place = line + sign * distance
        inside = jnp.logical_and(place >= 0, place < length)
        far = distance >= 1 if sign > 0 else distance >= 0
        return jnp.logical_and(inside, far)

    near = jnp.where(line == 0, 1, line - 1)
    final = chunks * (length - 1)
    slots = final + (half if quick else chunks)

    def cross_at(t):
        w = t + jnp.where(jnp.logical_and(end, t >= chunks + half), half, 0)
        return w // chunks, lax.rem(w, chunks)

    def late_at(t):
        return jnp.logical_and(end, t >= final), t - final + half

    def from_sibling(t):
        def take(s, k):
            arrived(s, k)
            to_peers(s, k)

        d, k = t // chunks + 1, lax.rem(t, chunks)
        e, m = cross_at(t)
        for sign in (-1, 1):
            pl.when(valid(sign, d))(lambda: take(index(line + sign * d, side, 1 - core), k))
            pl.when(valid(sign, e))(lambda: take(index(line + sign * e, 1 - side, 1 - core), m))
        is_late, m = late_at(t)
        pl.when(is_late)(lambda: take(index(near, 1 - side, 1 - core), m))

    def from_across(t):
        def take(s, k):
            arrived(s, k)
            share(s, k)
            to_peers(s, k)

        e, m = cross_at(t)
        for sign in (-1, 1):
            pl.when(valid(sign, e))(lambda: take(index(line + sign * e, 1 - side, core), m))
        is_late, n = late_at(t)
        pl.when(is_late)(lambda: take(index(near, 1 - side, core), n))

    def repeat(way, target, start):
        def one(k, _):
            copy(across, k, way, target).start()
            return 0

        lax.fori_loop(start, chunks, one, 0)

    def slot(t, _):
        d, k = t // chunks + 1, lax.rem(t, chunks)
        for sign, forward in ((-1, go_up), (1, go_down)):
            @pl.when(valid(sign, d))
            def _():
                s = index(line + sign * d, side, core)
                arrived(s, k)
                forward(s, k)
                by_line = jnp.logical_and(d == 1, k >= first_by_line(line, sign))
                pl.when(jnp.logical_not(by_line))(lambda: copy(s, k, 2, across).start())
                share(s, k)
                to_peers(s, k)

        from_across(t)
        pl.when(t >= 1)(lambda: from_sibling(t - 1))

        @pl.when(jnp.logical_and(k == chunks - 1, jnp.logical_and(has_up, d == jnp.maximum(line, 1))))
        def _():
            repeat(0, up, first_by_line(line + 1, -1))

        @pl.when(jnp.logical_and(k == chunks - 1, jnp.logical_and(has_down, d == jnp.maximum(length - 1 - line, 1))))
        def _():
            repeat(1, down, first_by_line(line - 1, 1))

        lax.fori_loop(done(t - 1), done(t), lambda v, _: work(v), 0)

        return 0

    def done(t):
        lag = jnp.full_like(t, chunks + 1)
        if quick:
            lag = jnp.where(jnp.logical_and(end, t >= final - half), chunks - half - (t - final), lag)
        return jnp.maximum(t + chunks + 1 - lag, 0)

    def end_slot(t, behind):
        from_sibling(t - 1)
        now = chunks + final - half + 1 + 2 * (t - final)
        lax.fori_loop(behind, now, lambda v, _: work(v), 0)
        was_late, m = late_at(t - 1)

        @pl.when(was_late)
        def _():
            late(m, 0)
            late(m, 1)

        from_across(t)
        return now

    def take_cols(s):
        @pl.when(owns_cols)
        def _():
            cols[s] = full[s, pl.ds(aligned, span), :]

        @pl.when(jnp.logical_not(owns_cols))
        def _():
            pltpu.make_async_copy(cols.at[s], cols.at[s], col_recv.at[s]).wait()

    def add_product(s, k):
        row = rows_of(s, k)
        right = cols[s]
        if span != tile:
            right = jnp.where(offset == aligned, right[:tile], right[span - tile:])
        product = lax.dot_general(
            full[s, row, :], right, (((1,), (1,)), ((), ())), preferred_element_type=jnp.float32
        )
        for b in range(out_ref.shape[0]):
            width = min(128, tile - b * 128)
            out_ref[b, row, :width] += product[:, b * 128:b * 128 + width]

    def work(v, lane=None):
        e, m = cross_at(v - chunks)

        def one(n, _):
            sign = 1 - 2 * (n // 4)
            cross = lax.rem(n // 2, 2)
            distance = jnp.where(cross == 1, e, v // chunks)
            k = jnp.where(cross == 1, m, lax.rem(v, chunks))
            place = line + sign * distance
            good = jnp.logical_and(place >= 0, place < length)
            good = jnp.logical_and(good, distance >= n // 4)
            good = jnp.logical_and(good, jnp.logical_or(cross == 0, v >= chunks))
            if lane is not None:
                good = jnp.logical_and(good, lax.rem(n, 2) == lane)

            @pl.when(good)
            def _():
                s = index(place, lax.rem(side + cross, 2), lax.rem(n, 2))
                pl.when(k == 0)(lambda: take_cols(s))
                add_product(s, k)

            return 0

        lax.fori_loop(0, 8, one, 0)
        return 0

    def late(k, lane):
        add_product(index(near, 1 - side, lane), k)

    def ready_own(k, _):
        s = index(line, side, 1 - core)
        arrived(s, k)
        to_peers(s, k)
        return 0

    lax.fori_loop(0, chunks, ready_own, 0)
    last = jnp.int32(slots - 1)
    if quick:
        lax.fori_loop(0, final, slot, 0)
        lax.fori_loop(final, slots, end_slot, done(jnp.int32(final - 1)))

        def finish(lane):
            work(last + chunks, lane)
            pl.when(end)(lambda: late(chunks - 1, lane))

        finish(core)
        from_sibling(last)
        finish(1 - core)
    else:
        lax.fori_loop(0, slots, slot, 0)
        from_sibling(last)
        lax.fori_loop(done(last), slots + chunks, lambda v, _: work(v), 0)

    def sent(s, way, count):
        ref = full.at[s, pl.ds(0, count * size)]
        pltpu.make_async_copy(ref, ref, send.at[way, s]).wait()

    def some_sent(s, way, count):
        pl.when(count == chunks)(lambda: sent(s, way, chunks))
        if quick:
            pl.when(count == half)(lambda: sent(s, way, half))

    def drain(place, _):
        straight, cross = index(place, side, core), index(place, 1 - side, core)
        sent(straight, 3, chunks)
        sent(cross, 3, chunks)
        beside = jnp.logical_or(place == line + 1, place == line - 1)
        sign = place - line
        some_sent(straight, 2, jnp.where(beside, first_by_line(line, sign), chunks))
        pl.when(jnp.logical_and(has_up, place <= line))(lambda: sent(straight, 0, chunks))
        pl.when(jnp.logical_and(has_down, place >= line))(lambda: sent(straight, 1, chunks))

        @pl.when(place == line)
        def _():
            pl.when(has_up)(lambda: some_sent(cross, 0, chunks - first_by_line(line + 1, -1)))
            pl.when(has_down)(lambda: some_sent(cross, 1, chunks - first_by_line(line - 1, 1)))

        return 0

    lax.fori_loop(0, length, drain, 0)

    @pl.when(owns_cols)
    def _():
        for n in range(len(peers)):
            pltpu.make_async_copy(cols, cols, col_send.at[n]).wait()

    for n in range(len(peers)):
        pltpu.make_async_copy(sums.at[i], sums.at[i], sum_send.at[n]).wait()


def flatten(tile, group, block, gram_ref, flat_ref, buffer, sem):
    groups = gram_ref.shape[1] // group
    wide = group * tile // 128
    scale = jnp.float32(1.0 / (MEMBERS - 1))
    for start in range(0, groups, block):
        many = min(block, groups - start)
        lane = lax.broadcasted_iota(jnp.int32, (many, 128), 1)
        for s in range(wide):
            value = None
            at = s * 128
            while at < (s + 1) * 128:
                r, c, to = at // tile, at % tile, at - s * 128
                count = min(tile - c, (s + 1) * 128 - at)
                shift = (to - c) % 128
                row = pl.ds(start * group + r, many, stride=group)
                here = gram_ref[c // 128, row, :]
                here = pltpu.roll(here, shift, 1) if shift else here
                if c % 128 + count > 128:
                    then = gram_ref[c // 128 + 1, row, :]
                    then = pltpu.roll(then, shift, 1) if shift else then
                    here = jnp.where(lane < to + 128 - c % 128, here, then)
                value = here if value is None else jnp.where(lane < to, value, here)
                at += count
            buffer[pl.ds(start * wide + s, many, stride=wide), :] = value * scale
        piece = pl.ds(start * wide, many * wide)
        pltpu.make_async_copy(buffer.at[piece], flat_ref.at[piece], sem).start()
    pltpu.make_async_copy(buffer, flat_ref, sem).wait()


def local(n_row, n_col, snapshots, area_weight):
    rows, depth = snapshots.shape
    tile = rows * n_row // n_col
    units = rows // 16
    chunks = max(n for n in range(1, MAX_CHUNKS + 1) if units % n == 0)
    size = rows // chunks
    length = n_col // 4
    ends = [*range(4), *range(n_col - 4, n_col)]
    whole = size % tile == 0 and tile % 16 == 0 and chunks % 4 == 0
    quick = length > 2 and whole and all(trigger(n_row, n_col, chunks, size, tile, me) < chunks // 2 for me in ends)
    span = tile + tile % 16
    blocks = -(-tile // 128)
    gram = pl.pallas_call(
        functools.partial(gather_gram, n_row, n_col, chunks, quick, tile),
        out_shape=jax.ShapeDtypeStruct((blocks, rows, 128), jnp.float32),
        in_specs=[pl.BlockSpec(memory_space=pltpu.VMEM)] * 2,
        out_specs=pl.BlockSpec(memory_space=pltpu.VMEM),
        scratch_shapes=[
            pltpu.VMEM((n_col, rows, depth), jnp.bfloat16),
            pltpu.VMEM((n_col, span, depth), jnp.bfloat16),
            pltpu.VMEM((n_row, 8, depth), jnp.float32),
            pltpu.SemaphoreType.DMA((n_col, chunks)),
            pltpu.SemaphoreType.DMA((4, n_col)),
            pltpu.SemaphoreType.DMA((n_col,)),
            pltpu.SemaphoreType.DMA((max(n_row - 1, 1),)),
            pltpu.SemaphoreType.DMA((n_row,)),
            pltpu.SemaphoreType.DMA((max(n_row - 1, 1),)),
        ],
        compiler_params=pltpu.CompilerParams(
            collective_id=0, has_side_effects=True, vmem_limit_bytes=44 * 2**20
        ),
        name="gather_gram",
    )(snapshots, area_weight.reshape(1, depth))
    group = 8
    while group * tile % 128:
        group *= 2
    groups = rows // group
    block = (groups // PIECES + 7) // 8 * 8
    flat_shape = (groups * group * tile // 128, 128)
    flat = pl.pallas_call(
        functools.partial(flatten, tile, group, block),
        out_shape=jax.ShapeDtypeStruct(flat_shape, jnp.float32),
        in_specs=[pl.BlockSpec(memory_space=pltpu.VMEM)],
        out_specs=pl.BlockSpec(memory_space=pl.ANY),
        scratch_shapes=[pltpu.VMEM(flat_shape, jnp.float32), pltpu.SemaphoreType.DMA],
        compiler_params=pltpu.CompilerParams(vmem_limit_bytes=24 * 2**20),
        name="flatten",
    )(gram)
    return flat.reshape(1, 1, rows * tile)


def solution(mesh):
    placed = (P("mrow", "pcol"), P("pcol"))
    return jax.shard_map(
        functools.partial(local, mesh.shape["mrow"], mesh.shape["pcol"]),
        mesh=mesh, in_specs=placed, out_specs=P("mrow", "pcol", None), check_vma=False,
    )
```

```python
import functools

import jax
import jax.numpy as jnp
from jax import lax
from jax.experimental import pallas as pl
from jax.experimental.pallas import tpu as pltpu
from jax.sharding import PartitionSpec as P

MEMBERS = 7424
MAX_CHUNKS = 4
PIECE = 80
MESH = pl.DeviceIdType.MESH


def trigger(n_row, n_col, chunks, size, tile, me):
    ratio = n_col // n_row
    root = me // ratio
    first = me % ratio * tile // 16 * 16
    last = first + tile + tile % 16 - 1
    up, down = last // size, chunks - 1 - first // size
    if isinstance(me, int):
        return down if 2 * root >= n_row else up
    return jnp.where(2 * root >= n_row, down, up)


def gather_gram(
    n_row, n_col, chunks, quick, tile, group, x_ref, weight_ref, out_ref, *rest,
):
    half_ref = rest[0] if quick else None
    full, cols, sums, recv, send, col_recv, col_send, sum_recv, sum_send = rest[1:] if quick else rest
    rows, depth = x_ref.shape
    length = n_col // 4
    size = rows // chunks
    half = chunks // 2
    span = cols.shape[1]
    i = lax.axis_index("mrow")
    me = lax.axis_index("pcol")
    core = lax.rem(me, 2)
    side = lax.rem(me // 2, 2)
    line = me // 4
    ratio = n_col // n_row
    root = me // ratio
    offset = lax.rem(me, ratio) * tile
    aligned = pl.multiple_of(offset // 16 * 16, 16)
    my_chunk = trigger(n_row, n_col, chunks, size, tile, me)
    backward = 2 * i >= n_row

    def index(where, which, own):
        return (where * 2 + which) * 2 + own

    up, down = index(line + 1, side, core), index(line - 1, side, core)
    across, sibling = index(line, 1 - side, core), index(line, side, 1 - core)
    has_up, has_down = line + 1 < length, line >= 1
    peers = [lax.rem(i + step, n_row) for step in range(1, n_row)]
    owns_cols = root == i

    def is_end(place):
        return jnp.logical_or(place == 0, place == length - 1)

    def first_by_line(place, sign):
        if not quick:
            return jnp.int32(chunks)
        return jnp.where(is_end(place), half, jnp.where(is_end(place + sign), 0, chunks))

    end = is_end(line) if quick else line < 0

    barrier = pltpu.get_barrier_semaphore()

    def greet(row, col):
        pl.semaphore_signal(barrier, inc=1, device_id=(row, col), device_id_type=MESH)

    pl.when(has_up)(lambda: greet(i, up))
    pl.when(has_down)(lambda: greet(i, down))
    greet(i, across)
    greet(i, sibling)
    for peer in peers:
        greet(peer, me)

    def add_up(k, total):
        block = x_ref[pl.ds(pl.multiple_of(k * size, 16), size), :].astype(jnp.float32)
        return total + jnp.sum(block.reshape(size // 8, 8, depth), axis=0)

    sums[i] = lax.fori_loop(0, chunks, add_up, jnp.zeros((8, depth), jnp.float32))
    pl.semaphore_wait(barrier, 2 + len(peers) + has_up.astype(jnp.int32) + has_down.astype(jnp.int32))

    def swapped(s, k):
        if not quick:
            return k
        swap = jnp.logical_and((lax.rem(s // 2, 2) == 0) != backward, k < half)
        return jnp.where(swap, lax.rem(k + half // 2, half), k)

    def rows_of(s, k):
        at = swapped(s, k)
        at = jnp.where(backward, chunks - 1 - at, at)
        return pl.ds(pl.multiple_of(at * size, 16), size)

    def part(s, k):
        return full.at[s, rows_of(s, k)]

    def copy(s, k, way, target):
        return pltpu.make_async_remote_copy(
            src_ref=part(s, k), dst_ref=part(s, k), send_sem=send.at[way, s], recv_sem=recv.at[s, k],
            device_id=(i, target), device_id_type=MESH,
        )

    def col_copy(s, n):
        return pltpu.make_async_remote_copy(
            src_ref=full.at[s, pl.ds(aligned, span)], dst_ref=cols.at[s], send_sem=col_send.at[n],
            recv_sem=col_recv.at[s], device_id=(peers[n], me), device_id_type=MESH,
        )

    def arrived(s, k):
        pltpu.make_async_copy(part(s, k), part(s, k), recv.at[s, k]).wait()

    def share(s, k):
        copy(s, k, 3, sibling).start()

    def to_peers(s, k):
        @pl.when(jnp.logical_and(owns_cols, swapped(s, k) == my_chunk))
        def _():
            for n in range(len(peers)):
                col_copy(s, n).start()

    def go_up(s, k):
        pl.when(has_up)(lambda: copy(s, k, 0, up).start())

    def go_down(s, k):
        pl.when(has_down)(lambda: copy(s, k, 1, down).start())

    def sum_copy(n):
        return pltpu.make_async_remote_copy(
            src_ref=sums.at[i], dst_ref=sums.at[i], send_sem=sum_send.at[n], recv_sem=sum_recv.at[i],
            device_id=(peers[n], me), device_id_type=MESH,
        )

    for n in range(len(peers)):
        sum_copy(n).start()
    out_ref[...] = jnp.zeros_like(out_ref)
    for peer in peers:
        pltpu.make_async_copy(sums.at[peer], sums.at[peer], sum_recv.at[peer]).wait()
    mean = jnp.sum(jnp.sum(sums[...], axis=0), axis=0, keepdims=True) / MEMBERS
    root_weight = jnp.sqrt(weight_ref[...])

    def center(k):
        row = rows_of(me, k)
        full[me, row, :] = ((x_ref[row, :].astype(jnp.float32) - mean) * root_weight).astype(jnp.bfloat16)

    def own(k, _):
        pl.when(k + 1 < chunks)(lambda: center(k + 1))
        copy(me, k, 2, across).start()
        go_up(me, k)
        go_down(me, k)
        share(me, k)
        to_peers(me, k)
        return 0

    center(0)
    lax.fori_loop(0, chunks, own, 0)

    def valid(sign, distance):
        place = line + sign * distance
        inside = jnp.logical_and(place >= 0, place < length)
        far = distance >= 1 if sign > 0 else distance >= 0
        return jnp.logical_and(inside, far)

    near = jnp.where(line == 0, 1, line - 1)
    final = chunks * (length - 1)
    slots = final + (half if quick else chunks)

    def cross_at(t):
        w = t + jnp.where(jnp.logical_and(end, t >= chunks + half), half, 0)
        return w // chunks, lax.rem(w, chunks)

    def late_at(t):
        return jnp.logical_and(end, t >= final), t - final + half

    def from_sibling(t):
        def take(s, k):
            arrived(s, k)
            to_peers(s, k)

        d, k = t // chunks + 1, lax.rem(t, chunks)
        e, m = cross_at(t)
        for sign in (-1, 1):
            pl.when(valid(sign, d))(lambda: take(index(line + sign * d, side, 1 - core), k))
            pl.when(valid(sign, e))(lambda: take(index(line + sign * e, 1 - side, 1 - core), m))
        is_late, m = late_at(t)
        pl.when(is_late)(lambda: take(index(near, 1 - side, 1 - core), m))

    def from_across(t):
        def take(s, k):
            arrived(s, k)
            share(s, k)
            to_peers(s, k)

        e, m = cross_at(t)
        for sign in (-1, 1):
            pl.when(valid(sign, e))(lambda: take(index(line + sign * e, 1 - side, core), m))
        is_late, n = late_at(t)
        pl.when(is_late)(lambda: take(index(near, 1 - side, core), n))

    def repeat(way, target, start):
        def one(k, _):
            copy(across, k, way, target).start()
            return 0

        lax.fori_loop(start, chunks, one, 0)

    def slot(t, _):
        d, k = t // chunks + 1, lax.rem(t, chunks)
        for sign, forward in ((-1, go_up), (1, go_down)):
            @pl.when(valid(sign, d))
            def _():
                s = index(line + sign * d, side, core)
                arrived(s, k)
                forward(s, k)
                by_line = jnp.logical_and(d == 1, k >= first_by_line(line, sign))
                pl.when(jnp.logical_not(by_line))(lambda: copy(s, k, 2, across).start())
                share(s, k)
                to_peers(s, k)

        from_across(t)
        pl.when(t >= 1)(lambda: from_sibling(t - 1))

        @pl.when(jnp.logical_and(k == chunks - 1, jnp.logical_and(has_up, d == jnp.maximum(line, 1))))
        def _():
            repeat(0, up, first_by_line(line + 1, -1))

        @pl.when(jnp.logical_and(k == chunks - 1, jnp.logical_and(has_down, d == jnp.maximum(length - 1 - line, 1))))
        def _():
            repeat(1, down, first_by_line(line - 1, 1))

        lax.fori_loop(done(t - 1), done(t), lambda v, _: work(v), 0)

        return 0

    def done(t):
        lag = jnp.full_like(t, chunks + 1)
        if quick:
            lag = jnp.where(jnp.logical_and(end, t >= final - half), chunks - half - (t - final), lag)
        return jnp.maximum(t + chunks + 1 - lag, 0)

    def end_slot(t, behind):
        from_sibling(t - 1)
        now = chunks + final - half + 1 + 2 * (t - final)
        lax.fori_loop(behind, now, lambda v, _: work(v), 0)
        was_late, m = late_at(t - 1)

        @pl.when(was_late)
        def _():
            late(m, 0)
            late(m, 1)

        @pl.when(t == slots - 1)
        def _():
            groups = rows // group // 2
            start = jnp.where(backward, groups, 0)
            flatten_rows(tile, group, out_ref, start, groups, half_ref, 0)

        from_across(t)
        return now

    def take_cols(s):
        @pl.when(owns_cols)
        def _():
            cols[s] = full[s, pl.ds(aligned, span), :]

        @pl.when(jnp.logical_not(owns_cols))
        def _():
            pltpu.make_async_copy(cols.at[s], cols.at[s], col_recv.at[s]).wait()

    def add_product(s, k):
        row = rows_of(s, k)
        right = cols[s]
        if span != tile:
            right = jnp.where(offset == aligned, right[:tile], right[span - tile:])
        product = lax.dot_general(
            full[s, row, :], right, (((1,), (1,)), ((), ())), preferred_element_type=jnp.float32
        )
        for b in range(out_ref.shape[0]):
            width = min(128, tile - b * 128)
            out_ref[b, row, :width] += product[:, b * 128:b * 128 + width]

    def work(v, lane=None):
        e, m = cross_at(v - chunks)

        def one(n, _):
            sign = 1 - 2 * (n // 4)
            cross = lax.rem(n // 2, 2)
            distance = jnp.where(cross == 1, e, v // chunks)
            k = jnp.where(cross == 1, m, lax.rem(v, chunks))
            place = line + sign * distance
            good = jnp.logical_and(place >= 0, place < length)
            good = jnp.logical_and(good, distance >= n // 4)
            good = jnp.logical_and(good, jnp.logical_or(cross == 0, v >= chunks))
            if lane is not None:
                good = jnp.logical_and(good, lax.rem(n, 2) == lane)

            @pl.when(good)
            def _():
                s = index(place, lax.rem(side + cross, 2), lax.rem(n, 2))
                pl.when(k == 0)(lambda: take_cols(s))
                add_product(s, k)

            return 0

        lax.fori_loop(0, 8, one, 0)
        return 0

    def late(k, lane):
        add_product(index(near, 1 - side, lane), k)

    def ready_own(k, _):
        s = index(line, side, 1 - core)
        arrived(s, k)
        to_peers(s, k)
        return 0

    lax.fori_loop(0, chunks, ready_own, 0)
    last = jnp.int32(slots - 1)
    if quick:
        lax.fori_loop(0, final, slot, 0)
        lax.fori_loop(final, slots, end_slot, done(jnp.int32(final - 1)))

        def finish(lane):
            work(last + chunks, lane)
            pl.when(end)(lambda: late(chunks - 1, lane))

        finish(core)
        from_sibling(last)
        finish(1 - core)
    else:
        lax.fori_loop(0, slots, slot, 0)
        from_sibling(last)
        lax.fori_loop(done(last), slots + chunks, lambda v, _: work(v), 0)

    def sent(s, way, count):
        ref = full.at[s, pl.ds(0, count * size)]
        pltpu.make_async_copy(ref, ref, send.at[way, s]).wait()

    def some_sent(s, way, count):
        pl.when(count == chunks)(lambda: sent(s, way, chunks))
        if quick:
            pl.when(count == half)(lambda: sent(s, way, half))

    def drain(place, _):
        straight, cross = index(place, side, core), index(place, 1 - side, core)
        sent(straight, 3, chunks)
        sent(cross, 3, chunks)
        beside = jnp.logical_or(place == line + 1, place == line - 1)
        sign = place - line
        some_sent(straight, 2, jnp.where(beside, first_by_line(line, sign), chunks))
        pl.when(jnp.logical_and(has_up, place <= line))(lambda: sent(straight, 0, chunks))
        pl.when(jnp.logical_and(has_down, place >= line))(lambda: sent(straight, 1, chunks))

        @pl.when(place == line)
        def _():
            pl.when(has_up)(lambda: some_sent(cross, 0, chunks - first_by_line(line + 1, -1)))
            pl.when(has_down)(lambda: some_sent(cross, 1, chunks - first_by_line(line - 1, 1)))

        return 0

    lax.fori_loop(0, length, drain, 0)

    @pl.when(owns_cols)
    def _():
        for n in range(len(peers)):
            pltpu.make_async_copy(cols, cols, col_send.at[n]).wait()

    for n in range(len(peers)):
        pltpu.make_async_copy(sums.at[i], sums.at[i], sum_send.at[n]).wait()


def flatten_rows(tile, group, gram_ref, start, many, flat_ref, to_row):
    wide = group * tile // 128
    scale = jnp.float32(1.0 / (MEMBERS - 1))
    first = start * group if isinstance(start, int) else pl.multiple_of(start * group, group)
    lane = lax.broadcasted_iota(jnp.int32, (many, 128), 1)
    for s in range(wide):
        value = None
        at = s * 128
        while at < (s + 1) * 128:
            r, c, to = at // tile, at % tile, at - s * 128
            count = min(tile - c, (s + 1) * 128 - at)
            shift = (to - c) % 128
            row = pl.ds(first + r, many, stride=group)
            here = gram_ref[c // 128, row, :]
            here = pltpu.roll(here, shift, 1) if shift else here
            if c % 128 + count > 128:
                then = gram_ref[c // 128 + 1, row, :]
                then = pltpu.roll(then, shift, 1) if shift else then
                here = jnp.where(lane < to + 128 - c % 128, here, then)
            value = here if value is None else jnp.where(lane < to, value, here)
            at += count
        flat_ref[pl.ds(to_row + s, many, stride=wide), :] = value * scale


def flatten(n_row, tile, group, gram_ref, *rest):
    groups = gram_ref.shape[1] // group
    wide = group * tile // 128
    if len(rest) == 5:
        half_ref, flat_ref, buffer, sem, half_sem = rest
        groups //= 2
        backward = 2 * lax.axis_index("mrow") >= n_row
        start, done = jnp.where(backward, 0, groups), jnp.where(backward, groups, 0)
        half_copy = pltpu.make_async_copy(
            half_ref, flat_ref.at[pl.ds(pl.multiple_of(done * wide, 8), groups * wide)], half_sem
        )
        half_copy.start()
    else:
        flat_ref, buffer, sem = rest
        start, half_copy = 0, None
    for piece in range(0, groups, PIECE):
        many = min(PIECE, groups - piece)
        flatten_rows(tile, group, gram_ref, start + piece, many, buffer, piece * wide)
        target = (start + piece) * wide
        target = target if half_copy is None else pl.multiple_of(target, 8)
        pltpu.make_async_copy(
            buffer.at[pl.ds(piece * wide, many * wide)], flat_ref.at[pl.ds(target, many * wide)], sem
        ).start()
    pltpu.make_async_copy(buffer, flat_ref.at[pl.ds(0, groups * wide)], sem).wait()
    if half_copy is not None:
        half_copy.wait()


def local(n_row, n_col, snapshots, area_weight):
    rows, depth = snapshots.shape
    tile = rows * n_row // n_col
    units = rows // 16
    chunks = max(n for n in range(1, MAX_CHUNKS + 1) if units % n == 0)
    size = rows // chunks
    length = n_col // 4
    ends = [*range(4), *range(n_col - 4, n_col)]
    whole = size % tile == 0 and tile % 16 == 0 and chunks % 4 == 0
    quick = length > 2 and whole and all(trigger(n_row, n_col, chunks, size, tile, me) < chunks // 2 for me in ends)
    span = tile + tile % 16
    blocks = -(-tile // 128)
    group = 8
    while group * tile % 128:
        group *= 2
    flat_shape = (rows * tile // 128, 128)
    half_shape = (flat_shape[0] // 2, 128)
    quick = quick and rows % (16 * group) == 0 and half_shape[0] % 8 == 0
    shapes = [(blocks, rows, 128)] + [half_shape] * quick
    parts = pl.pallas_call(
        functools.partial(gather_gram, n_row, n_col, chunks, quick, tile, group),
        out_shape=[jax.ShapeDtypeStruct(shape, jnp.float32) for shape in shapes],
        in_specs=[pl.BlockSpec(memory_space=pltpu.VMEM)] * 2,
        out_specs=[pl.BlockSpec(memory_space=pltpu.VMEM)] * len(shapes),
        scratch_shapes=[
            pltpu.VMEM((n_col, rows, depth), jnp.bfloat16),
            pltpu.VMEM((n_col, span, depth), jnp.bfloat16),
            pltpu.VMEM((n_row, 8, depth), jnp.float32),
            pltpu.SemaphoreType.DMA((n_col, chunks)),
            pltpu.SemaphoreType.DMA((4, n_col)),
            pltpu.SemaphoreType.DMA((n_col,)),
            pltpu.SemaphoreType.DMA((max(n_row - 1, 1),)),
            pltpu.SemaphoreType.DMA((n_row,)),
            pltpu.SemaphoreType.DMA((max(n_row - 1, 1),)),
        ],
        compiler_params=pltpu.CompilerParams(
            collective_id=0, has_side_effects=True, vmem_limit_bytes=38 * 2**20
        ),
        name="gather_gram",
    )(snapshots, area_weight.reshape(1, depth))
    flat = pl.pallas_call(
        functools.partial(flatten, n_row, tile, group),
        out_shape=jax.ShapeDtypeStruct(flat_shape, jnp.float32),
        in_specs=[pl.BlockSpec(memory_space=pltpu.VMEM)] * len(shapes),
        out_specs=pl.BlockSpec(memory_space=pl.ANY),
        scratch_shapes=[
            pltpu.VMEM(half_shape if quick else flat_shape, jnp.float32),
            *[pltpu.SemaphoreType.DMA] * len(shapes),
        ],
        compiler_params=pltpu.CompilerParams(vmem_limit_bytes=16 * 2**20),
        name="flatten",
    )(*parts)
    return flat.reshape(1, 1, rows * tile)


def solution(mesh):
    placed = (P("mrow", "pcol"), P("pcol"))
    return jax.shard_map(
        functools.partial(local, mesh.shape["mrow"], mesh.shape["pcol"]),
        mesh=mesh, in_specs=placed, out_specs=P("mrow", "pcol", None), check_vma=False,
    )
```

```python
import functools

import jax
import jax.numpy as jnp
from jax import lax
from jax.experimental import pallas as pl
from jax.experimental.pallas import tpu as pltpu
from jax.sharding import PartitionSpec as P

MAX_CHUNKS = 4
PIECE = 80
MESH = pl.DeviceIdType.MESH


def trigger(n_row, n_col, chunks, size, tile, me):
    ratio = n_col // n_row
    root = me // ratio
    first = me % ratio * tile // 16 * 16
    last = first + tile + tile % 16 - 1
    up, down = last // size, chunks - 1 - first // size
    if isinstance(me, int):
        return down if 2 * root >= n_row else up
    return jnp.where(2 * root >= n_row, down, up)


def gather_gram(
    n_row, n_col, chunks, quick, tile, group, x_ref, weight_ref, out_ref, *rest,
):
    half_ref = rest[0] if quick else None
    full, cols, sums, recv, send, col_recv, col_send, sum_recv, sum_send = rest[1:] if quick else rest
    rows, depth = x_ref.shape
    length = n_col // 4
    size = rows // chunks
    half = chunks // 2
    span = cols.shape[1]
    i = lax.axis_index("mrow")
    me = lax.axis_index("pcol")
    core = lax.rem(me, 2)
    side = lax.rem(me // 2, 2)
    line = me // 4
    ratio = n_col // n_row
    root = me // ratio
    offset = lax.rem(me, ratio) * tile
    aligned = pl.multiple_of(offset // 16 * 16, 16)
    my_chunk = trigger(n_row, n_col, chunks, size, tile, me)
    backward = 2 * i >= n_row

    def index(where, which, own):
        return (where * 2 + which) * 2 + own

    up, down = index(line + 1, side, core), index(line - 1, side, core)
    across, sibling = index(line, 1 - side, core), index(line, side, 1 - core)
    has_up, has_down = line + 1 < length, line >= 1
    peers = [lax.rem(i + step, n_row) for step in range(1, n_row)]
    owns_cols = root == i

    def is_end(place):
        return jnp.logical_or(place == 0, place == length - 1)

    def first_by_line(place, sign):
        if not quick:
            return jnp.int32(chunks)
        return jnp.where(is_end(place), half, jnp.where(is_end(place + sign), 0, chunks))

    end = is_end(line) if quick else line < 0

    barrier = pltpu.get_barrier_semaphore()

    def greet(row, col):
        pl.semaphore_signal(barrier, inc=1, device_id=(row, col), device_id_type=MESH)

    pl.when(has_up)(lambda: greet(i, up))
    pl.when(has_down)(lambda: greet(i, down))
    greet(i, across)
    greet(i, sibling)
    for peer in peers:
        greet(peer, me)

    def add_up(k, total):
        block = x_ref[pl.ds(pl.multiple_of(k * size, 16), size), :].astype(jnp.float32)
        return total + jnp.sum(block.reshape(size // 8, 8, depth), axis=0)

    sums[i] = lax.fori_loop(0, chunks, add_up, jnp.zeros((8, depth), jnp.float32))
    pl.semaphore_wait(barrier, 2 + len(peers) + has_up.astype(jnp.int32) + has_down.astype(jnp.int32))

    def swapped(s, k):
        if not quick:
            return k
        swap = jnp.logical_and((lax.rem(s // 2, 2) == 0) != backward, k < half)
        return jnp.where(swap, lax.rem(k + half // 2, half), k)

    def rows_of(s, k):
        at = swapped(s, k)
        at = jnp.where(backward, chunks - 1 - at, at)
        return pl.ds(pl.multiple_of(at * size, 16), size)

    def part(s, k):
        return full.at[s, rows_of(s, k)]

    def copy(s, k, way, target):
        return pltpu.make_async_remote_copy(
            src_ref=part(s, k), dst_ref=part(s, k), send_sem=send.at[way, s], recv_sem=recv.at[s, k],
            device_id=(i, target), device_id_type=MESH,
        )

    def col_copy(s, n):
        return pltpu.make_async_remote_copy(
            src_ref=full.at[s, pl.ds(aligned, span)], dst_ref=cols.at[s], send_sem=col_send.at[n],
            recv_sem=col_recv.at[s], device_id=(peers[n], me), device_id_type=MESH,
        )

    def arrived(s, k):
        pltpu.make_async_copy(part(s, k), part(s, k), recv.at[s, k]).wait()

    def share(s, k):
        copy(s, k, 3, sibling).start()

    def to_peers(s, k):
        @pl.when(jnp.logical_and(owns_cols, swapped(s, k) == my_chunk))
        def _():
            for n in range(len(peers)):
                col_copy(s, n).start()

    def go_up(s, k):
        pl.when(has_up)(lambda: copy(s, k, 0, up).start())

    def go_down(s, k):
        pl.when(has_down)(lambda: copy(s, k, 1, down).start())

    def sum_copy(n):
        return pltpu.make_async_remote_copy(
            src_ref=sums.at[i], dst_ref=sums.at[i], send_sem=sum_send.at[n], recv_sem=sum_recv.at[i],
            device_id=(peers[n], me), device_id_type=MESH,
        )

    for n in range(len(peers)):
        sum_copy(n).start()
    out_ref[...] = jnp.zeros_like(out_ref)
    for peer in peers:
        pltpu.make_async_copy(sums.at[peer], sums.at[peer], sum_recv.at[peer]).wait()
    mean = jnp.sum(jnp.sum(sums[...], axis=0), axis=0, keepdims=True) / (rows * n_row)
    root_weight = jnp.sqrt(weight_ref[...])

    def center(k):
        row = rows_of(me, k)
        full[me, row, :] = ((x_ref[row, :].astype(jnp.float32) - mean) * root_weight).astype(jnp.bfloat16)

    def own(k, _):
        pl.when(k + 1 < chunks)(lambda: center(k + 1))
        copy(me, k, 2, across).start()
        go_up(me, k)
        go_down(me, k)
        share(me, k)
        to_peers(me, k)
        return 0

    center(0)
    lax.fori_loop(0, chunks, own, 0)

    def valid(sign, distance):
        place = line + sign * distance
        inside = jnp.logical_and(place >= 0, place < length)
        far = distance >= 1 if sign > 0 else distance >= 0
        return jnp.logical_and(inside, far)

    near = jnp.where(line == 0, 1, line - 1)
    final = chunks * (length - 1)
    slots = final + (half if quick else chunks)

    def cross_at(t):
        w = t + jnp.where(jnp.logical_and(end, t >= chunks + half), half, 0)
        return w // chunks, lax.rem(w, chunks)

    def late_at(t):
        return jnp.logical_and(end, t >= final), t - final + half

    def from_sibling(t):
        def take(s, k):
            arrived(s, k)
            to_peers(s, k)

        d, k = t // chunks + 1, lax.rem(t, chunks)
        e, m = cross_at(t)
        for sign in (-1, 1):
            pl.when(valid(sign, d))(lambda: take(index(line + sign * d, side, 1 - core), k))
            pl.when(valid(sign, e))(lambda: take(index(line + sign * e, 1 - side, 1 - core), m))
        is_late, m = late_at(t)
        pl.when(is_late)(lambda: take(index(near, 1 - side, 1 - core), m))

    def from_across(t):
        def take(s, k):
            arrived(s, k)
            share(s, k)
            to_peers(s, k)

        e, m = cross_at(t)
        for sign in (-1, 1):
            pl.when(valid(sign, e))(lambda: take(index(line + sign * e, 1 - side, core), m))
        is_late, n = late_at(t)
        pl.when(is_late)(lambda: take(index(near, 1 - side, core), n))

    def repeat(way, target, start):
        def one(k, _):
            copy(across, k, way, target).start()
            return 0

        lax.fori_loop(start, chunks, one, 0)

    def slot(t, _):
        d, k = t // chunks + 1, lax.rem(t, chunks)
        for sign, forward in ((-1, go_up), (1, go_down)):
            @pl.when(valid(sign, d))
            def _():
                s = index(line + sign * d, side, core)
                arrived(s, k)
                forward(s, k)
                by_line = jnp.logical_and(d == 1, k >= first_by_line(line, sign))
                pl.when(jnp.logical_not(by_line))(lambda: copy(s, k, 2, across).start())
                share(s, k)
                to_peers(s, k)

        from_across(t)
        pl.when(t >= 1)(lambda: from_sibling(t - 1))

        @pl.when(jnp.logical_and(k == chunks - 1, jnp.logical_and(has_up, d == jnp.maximum(line, 1))))
        def _():
            repeat(0, up, first_by_line(line + 1, -1))

        @pl.when(jnp.logical_and(k == chunks - 1, jnp.logical_and(has_down, d == jnp.maximum(length - 1 - line, 1))))
        def _():
            repeat(1, down, first_by_line(line - 1, 1))

        lax.fori_loop(done(t - 1), done(t), lambda v, _: work(v), 0)

        return 0

    def done(t):
        lag = jnp.full_like(t, chunks + 1)
        if quick:
            lag = jnp.where(jnp.logical_and(end, t >= final - half), chunks - half - (t - final), lag)
        return jnp.maximum(t + chunks + 1 - lag, 0)

    def end_slot(t, behind):
        from_sibling(t - 1)
        now = chunks + final - half + 1 + 2 * (t - final)
        lax.fori_loop(behind, now, lambda v, _: work(v), 0)
        was_late, m = late_at(t - 1)

        @pl.when(was_late)
        def _():
            late(m, 0)
            late(m, 1)

        @pl.when(t == slots - 1)
        def _():
            groups = rows // group // 2
            start = jnp.where(backward, groups, 0)
            flatten_rows(rows * n_row, tile, group, out_ref, start, groups, half_ref, 0)

        from_across(t)
        return now

    def take_cols(s):
        @pl.when(owns_cols)
        def _():
            cols[s] = full[s, pl.ds(aligned, span), :]

        @pl.when(jnp.logical_not(owns_cols))
        def _():
            pltpu.make_async_copy(cols.at[s], cols.at[s], col_recv.at[s]).wait()

    def add_product(s, k):
        row = rows_of(s, k)
        right = cols[s]
        if span != tile:
            right = jnp.where(offset == aligned, right[:tile], right[span - tile:])
        product = lax.dot_general(
            full[s, row, :], right, (((1,), (1,)), ((), ())), preferred_element_type=jnp.float32
        )
        for b in range(out_ref.shape[0]):
            width = min(128, tile - b * 128)
            out_ref[b, row, :width] += product[:, b * 128:b * 128 + width]

    def work(v, lane=None):
        e, m = cross_at(v - chunks)

        def one(n, _):
            sign = 1 - 2 * (n // 4)
            cross = lax.rem(n // 2, 2)
            distance = jnp.where(cross == 1, e, v // chunks)
            k = jnp.where(cross == 1, m, lax.rem(v, chunks))
            place = line + sign * distance
            good = jnp.logical_and(place >= 0, place < length)
            good = jnp.logical_and(good, distance >= n // 4)
            good = jnp.logical_and(good, jnp.logical_or(cross == 0, v >= chunks))
            if lane is not None:
                good = jnp.logical_and(good, lax.rem(n, 2) == lane)

            @pl.when(good)
            def _():
                s = index(place, lax.rem(side + cross, 2), lax.rem(n, 2))
                pl.when(k == 0)(lambda: take_cols(s))
                add_product(s, k)

            return 0

        lax.fori_loop(0, 8, one, 0)
        return 0

    def late(k, lane):
        add_product(index(near, 1 - side, lane), k)

    def ready_own(k, _):
        s = index(line, side, 1 - core)
        arrived(s, k)
        to_peers(s, k)
        return 0

    lax.fori_loop(0, chunks, ready_own, 0)
    last = jnp.int32(slots - 1)
    if quick:
        lax.fori_loop(0, final, slot, 0)
        lax.fori_loop(final, slots, end_slot, done(jnp.int32(final - 1)))

        def finish(lane):
            work(last + chunks, lane)
            pl.when(end)(lambda: late(chunks - 1, lane))

        finish(core)
        from_sibling(last)
        finish(1 - core)
    else:
        lax.fori_loop(0, slots, slot, 0)
        from_sibling(last)
        lax.fori_loop(done(last), slots + chunks, lambda v, _: work(v), 0)

    def sent(s, way, count):
        ref = full.at[s, pl.ds(0, count * size)]
        pltpu.make_async_copy(ref, ref, send.at[way, s]).wait()

    def some_sent(s, way, count):
        pl.when(count == chunks)(lambda: sent(s, way, chunks))
        if quick:
            pl.when(count == half)(lambda: sent(s, way, half))

    def drain(place, _):
        straight, cross = index(place, side, core), index(place, 1 - side, core)
        sent(straight, 3, chunks)
        sent(cross, 3, chunks)
        beside = jnp.logical_or(place == line + 1, place == line - 1)
        sign = place - line
        some_sent(straight, 2, jnp.where(beside, first_by_line(line, sign), chunks))
        pl.when(jnp.logical_and(has_up, place <= line))(lambda: sent(straight, 0, chunks))
        pl.when(jnp.logical_and(has_down, place >= line))(lambda: sent(straight, 1, chunks))

        @pl.when(place == line)
        def _():
            pl.when(has_up)(lambda: some_sent(cross, 0, chunks - first_by_line(line + 1, -1)))
            pl.when(has_down)(lambda: some_sent(cross, 1, chunks - first_by_line(line - 1, 1)))

        return 0

    lax.fori_loop(0, length, drain, 0)

    @pl.when(owns_cols)
    def _():
        for n in range(len(peers)):
            pltpu.make_async_copy(cols, cols, col_send.at[n]).wait()

    for n in range(len(peers)):
        pltpu.make_async_copy(sums.at[i], sums.at[i], sum_send.at[n]).wait()


def flatten_rows(members, tile, group, gram_ref, start, many, flat_ref, to_row):
    wide = group * tile // 128
    scale = jnp.float32(1.0 / (members - 1))
    first = start * group if isinstance(start, int) else pl.multiple_of(start * group, group)
    lane = lax.broadcasted_iota(jnp.int32, (many, 128), 1)
    for s in range(wide):
        value = None
        at = s * 128
        while at < (s + 1) * 128:
            r, c, to = at // tile, at % tile, at - s * 128
            count = min(tile - c, (s + 1) * 128 - at)
            shift = (to - c) % 128
            row = pl.ds(first + r, many, stride=group)
            here = gram_ref[c // 128, row, :]
            here = pltpu.roll(here, shift, 1) if shift else here
            if c % 128 + count > 128:
                then = gram_ref[c // 128 + 1, row, :]
                then = pltpu.roll(then, shift, 1) if shift else then
                here = jnp.where(lane < to + 128 - c % 128, here, then)
            value = here if value is None else jnp.where(lane < to, value, here)
            at += count
        flat_ref[pl.ds(to_row + s, many, stride=wide), :] = value * scale


def flatten(n_row, tile, group, gram_ref, *rest):
    members = gram_ref.shape[1] * n_row
    groups = gram_ref.shape[1] // group
    wide = group * tile // 128
    if len(rest) == 5:
        half_ref, flat_ref, buffer, sem, half_sem = rest
        groups //= 2
        backward = 2 * lax.axis_index("mrow") >= n_row
        start, done = jnp.where(backward, 0, groups), jnp.where(backward, groups, 0)
        half_copy = pltpu.make_async_copy(
            half_ref, flat_ref.at[pl.ds(pl.multiple_of(done * wide, 8), groups * wide)], half_sem
        )
        half_copy.start()
    else:
        flat_ref, buffer, sem = rest
        start, half_copy = 0, None
    for piece in range(0, groups, PIECE):
        many = min(PIECE, groups - piece)
        flatten_rows(members, tile, group, gram_ref, start + piece, many, buffer, piece * wide)
        target = (start + piece) * wide
        target = target if half_copy is None else pl.multiple_of(target, 8)
        pltpu.make_async_copy(
            buffer.at[pl.ds(piece * wide, many * wide)], flat_ref.at[pl.ds(target, many * wide)], sem
        ).start()
    pltpu.make_async_copy(buffer, flat_ref.at[pl.ds(0, groups * wide)], sem).wait()
    if half_copy is not None:
        half_copy.wait()


def local(n_row, n_col, snapshots, area_weight):
    rows, depth = snapshots.shape
    tile = rows * n_row // n_col
    units = rows // 16
    chunks = max(n for n in range(1, MAX_CHUNKS + 1) if units % n == 0)
    size = rows // chunks
    length = n_col // 4
    ends = [*range(4), *range(n_col - 4, n_col)]
    whole = size % tile == 0 and tile % 16 == 0 and chunks % 4 == 0
    quick = length > 2 and whole and all(trigger(n_row, n_col, chunks, size, tile, me) < chunks // 2 for me in ends)
    span = tile + tile % 16
    blocks = -(-tile // 128)
    group = 8
    while group * tile % 128:
        group *= 2
    flat_shape = (rows * tile // 128, 128)
    half_shape = (flat_shape[0] // 2, 128)
    quick = quick and rows % (16 * group) == 0 and half_shape[0] % 8 == 0
    shapes = [(blocks, rows, 128)] + [half_shape] * quick
    parts = pl.pallas_call(
        functools.partial(gather_gram, n_row, n_col, chunks, quick, tile, group),
        out_shape=[jax.ShapeDtypeStruct(shape, jnp.float32) for shape in shapes],
        in_specs=[pl.BlockSpec(memory_space=pltpu.VMEM)] * 2,
        out_specs=[pl.BlockSpec(memory_space=pltpu.VMEM)] * len(shapes),
        scratch_shapes=[
            pltpu.VMEM((n_col, rows, depth), jnp.bfloat16),
            pltpu.VMEM((n_col, span, depth), jnp.bfloat16),
            pltpu.VMEM((n_row, 8, depth), jnp.float32),
            pltpu.SemaphoreType.DMA((n_col, chunks)),
            pltpu.SemaphoreType.DMA((4, n_col)),
            pltpu.SemaphoreType.DMA((n_col,)),
            pltpu.SemaphoreType.DMA((max(n_row - 1, 1),)),
            pltpu.SemaphoreType.DMA((n_row,)),
            pltpu.SemaphoreType.DMA((max(n_row - 1, 1),)),
        ],
        compiler_params=pltpu.CompilerParams(
            collective_id=0, has_side_effects=True, vmem_limit_bytes=38 * 2**20
        ),
        name="gather_gram",
    )(snapshots, area_weight.reshape(1, depth))
    flat = pl.pallas_call(
        functools.partial(flatten, n_row, tile, group),
        out_shape=jax.ShapeDtypeStruct(flat_shape, jnp.float32),
        in_specs=[pl.BlockSpec(memory_space=pltpu.VMEM)] * len(shapes),
        out_specs=pl.BlockSpec(memory_space=pl.ANY),
        scratch_shapes=[
            pltpu.VMEM(half_shape if quick else flat_shape, jnp.float32),
            *[pltpu.SemaphoreType.DMA] * len(shapes),
        ],
        compiler_params=pltpu.CompilerParams(vmem_limit_bytes=16 * 2**20),
        name="flatten",
    )(*parts)
    return flat.reshape(1, 1, rows * tile)


def solution(mesh):
    placed = (P("mrow", "pcol"), P("pcol"))
    return jax.shard_map(
        functools.partial(local, mesh.shape["mrow"], mesh.shape["pcol"]),
        mesh=mesh, in_specs=placed, out_specs=P("mrow", "pcol", None), check_vma=False,
    )
```

```python
import functools

import jax
import jax.numpy as jnp
from jax import lax
from jax.experimental import pallas as pl
from jax.experimental.pallas import tpu as pltpu
from jax.sharding import PartitionSpec as P

MAX_CHUNKS = 4
PIECE = 80
MESH = pl.DeviceIdType.MESH


def trigger(n_row, n_col, chunks, size, tile, me):
    ratio = n_col // n_row
    root = me // ratio
    first = me % ratio * tile // 16 * 16
    last = first + tile + tile % 16 - 1
    up, down = last // size, chunks - 1 - first // size
    if isinstance(me, int):
        return down if 2 * root >= n_row else up
    return jnp.where(2 * root >= n_row, down, up)


def gather_gram(
    n_row, n_col, chunks, quick, tile, group, x_ref, weight_ref, out_ref, *rest,
):
    half_ref = rest[0] if quick else None
    full, cols, sums, recv, send, col_recv, col_send, sum_recv, sum_send = rest[1:] if quick else rest
    rows, depth = x_ref.shape
    length = n_col // 4
    size = rows // chunks
    half = chunks // 2
    span = cols.shape[1]
    i = lax.axis_index("mrow")
    me = lax.axis_index("pcol")
    core = lax.rem(me, 2)
    side = lax.rem(me // 2, 2)
    line = me // 4
    ratio = n_col // n_row
    root = me // ratio
    offset = lax.rem(me, ratio) * tile
    aligned = pl.multiple_of(offset // 16 * 16, 16)
    my_chunk = trigger(n_row, n_col, chunks, size, tile, me)
    backward = 2 * i >= n_row

    def index(where, which, own):
        return (where * 2 + which) * 2 + own

    up, down = index(line + 1, side, core), index(line - 1, side, core)
    across, sibling = index(line, 1 - side, core), index(line, side, 1 - core)
    has_up, has_down = line + 1 < length, line >= 1
    peers = [lax.rem(i + step, n_row) for step in range(1, n_row)]
    owns_cols = root == i

    def is_end(place):
        return jnp.logical_or(place == 0, place == length - 1)

    def first_by_line(place, sign):
        if not quick:
            return jnp.int32(chunks)
        return jnp.where(is_end(place), half, jnp.where(is_end(place + sign), 0, chunks))

    end = is_end(line) if quick else line < 0

    barrier = pltpu.get_barrier_semaphore()

    def greet(row, col):
        pl.semaphore_signal(barrier, inc=1, device_id=(row, col), device_id_type=MESH)

    pl.when(has_up)(lambda: greet(i, up))
    pl.when(has_down)(lambda: greet(i, down))
    greet(i, across)
    greet(i, sibling)
    for peer in peers:
        greet(peer, me)

    def add_up(k, total):
        block = x_ref[pl.ds(pl.multiple_of(k * size, 16), size), :].astype(jnp.float32)
        return total + jnp.sum(block.reshape(size // 8, 8, depth), axis=0)

    sums[i] = lax.fori_loop(0, chunks, add_up, jnp.zeros((8, depth), jnp.float32))
    pl.semaphore_wait(barrier, 2 + len(peers) + has_up.astype(jnp.int32) + has_down.astype(jnp.int32))

    def swapped(s, k):
        if not quick:
            return k
        swap = jnp.logical_and((lax.rem(s // 2, 2) == 0) != backward, k < half)
        return jnp.where(swap, lax.rem(k + half // 2, half), k)

    def rows_of(s, k):
        at = swapped(s, k)
        at = jnp.where(backward, chunks - 1 - at, at)
        return pl.ds(pl.multiple_of(at * size, 16), size)

    def part(s, k):
        return full.at[s, rows_of(s, k)]

    def copy(s, k, way, target):
        return pltpu.make_async_remote_copy(
            src_ref=part(s, k), dst_ref=part(s, k), send_sem=send.at[way, s], recv_sem=recv.at[s, k],
            device_id=(i, target), device_id_type=MESH,
        )

    def col_copy(s, n):
        return pltpu.make_async_remote_copy(
            src_ref=full.at[s, pl.ds(aligned, span)], dst_ref=cols.at[s], send_sem=col_send.at[n],
            recv_sem=col_recv.at[s], device_id=(peers[n], me), device_id_type=MESH,
        )

    def arrived(s, k):
        pltpu.make_async_copy(part(s, k), part(s, k), recv.at[s, k]).wait()

    def share(s, k):
        copy(s, k, 3, sibling).start()

    def to_peers(s, k):
        @pl.when(jnp.logical_and(owns_cols, swapped(s, k) == my_chunk))
        def _():
            for n in range(len(peers)):
                col_copy(s, n).start()

    def go_up(s, k):
        pl.when(has_up)(lambda: copy(s, k, 0, up).start())

    def go_down(s, k):
        pl.when(has_down)(lambda: copy(s, k, 1, down).start())

    def sum_copy(n):
        return pltpu.make_async_remote_copy(
            src_ref=sums.at[i], dst_ref=sums.at[i], send_sem=sum_send.at[n], recv_sem=sum_recv.at[i],
            device_id=(peers[n], me), device_id_type=MESH,
        )

    for n in range(len(peers)):
        sum_copy(n).start()
    out_ref[...] = jnp.zeros_like(out_ref)
    for peer in peers:
        pltpu.make_async_copy(sums.at[peer], sums.at[peer], sum_recv.at[peer]).wait()
    mean = jnp.sum(jnp.sum(sums[...], axis=0), axis=0, keepdims=True) / (rows * n_row)
    root_weight = jnp.sqrt(weight_ref[...])

    def center(k):
        row = rows_of(me, k)
        full[me, row, :] = ((x_ref[row, :].astype(jnp.float32) - mean) * root_weight).astype(jnp.bfloat16)

    def own(k, _):
        pl.when(k + 1 < chunks)(lambda: center(k + 1))
        copy(me, k, 2, across).start()
        go_up(me, k)
        go_down(me, k)
        share(me, k)
        to_peers(me, k)
        return 0

    center(0)
    lax.fori_loop(0, chunks, own, 0)

    def valid(sign, distance):
        place = line + sign * distance
        inside = jnp.logical_and(place >= 0, place < length)
        far = distance >= 1 if sign > 0 else distance >= 0
        return jnp.logical_and(inside, far)

    near = jnp.where(line == 0, 1, line - 1)
    final = chunks * (length - 1)
    slots = final + (half if quick else chunks)

    def cross_at(t):
        w = t + jnp.where(jnp.logical_and(end, t >= chunks + half), half, 0)
        return w // chunks, lax.rem(w, chunks)

    def late_at(t):
        return jnp.logical_and(end, t >= final), t - final + half

    def from_sibling(t):
        def take(s, k):
            arrived(s, k)
            to_peers(s, k)

        d, k = t // chunks + 1, lax.rem(t, chunks)
        e, m = cross_at(t)
        for sign in (-1, 1):
            pl.when(valid(sign, d))(lambda: take(index(line + sign * d, side, 1 - core), k))
            pl.when(valid(sign, e))(lambda: take(index(line + sign * e, 1 - side, 1 - core), m))
        is_late, m = late_at(t)
        pl.when(is_late)(lambda: take(index(near, 1 - side, 1 - core), m))

    def from_across(t):
        def take(s, k):
            arrived(s, k)
            share(s, k)
            to_peers(s, k)

        e, m = cross_at(t)
        for sign in (-1, 1):
            pl.when(valid(sign, e))(lambda: take(index(line + sign * e, 1 - side, core), m))
        is_late, n = late_at(t)
        pl.when(is_late)(lambda: take(index(near, 1 - side, core), n))

    def repeat(way, target, start):
        def one(k, _):
            copy(across, k, way, target).start()
            return 0

        lax.fori_loop(start, chunks, one, 0)

    def slot(t, _):
        d, k = t // chunks + 1, lax.rem(t, chunks)
        for sign, forward in ((-1, go_up), (1, go_down)):
            @pl.when(valid(sign, d))
            def _():
                s = index(line + sign * d, side, core)
                arrived(s, k)
                forward(s, k)
                by_line = jnp.logical_and(d == 1, k >= first_by_line(line, sign))
                pl.when(jnp.logical_not(by_line))(lambda: copy(s, k, 2, across).start())
                share(s, k)
                to_peers(s, k)

        from_across(t)
        pl.when(t >= 1)(lambda: from_sibling(t - 1))

        @pl.when(jnp.logical_and(k == chunks - 1, jnp.logical_and(has_up, d == jnp.maximum(line, 1))))
        def _():
            repeat(0, up, first_by_line(line + 1, -1))

        @pl.when(jnp.logical_and(k == chunks - 1, jnp.logical_and(has_down, d == jnp.maximum(length - 1 - line, 1))))
        def _():
            repeat(1, down, first_by_line(line - 1, 1))

        lax.fori_loop(done(t - 1), done(t), lambda v, _: work(v), 0)

        return 0

    def done(t):
        lag = jnp.full_like(t, chunks + 1)
        if quick:
            lag = jnp.where(jnp.logical_and(end, t >= final - half), chunks - half - (t - final), lag)
        return jnp.maximum(t + chunks + 1 - lag, 0)

    def end_slot(t, behind):
        from_sibling(t - 1)
        now = chunks + final - half + 1 + 2 * (t - final)
        lax.fori_loop(behind, now, lambda v, _: work(v), 0)
        was_late, m = late_at(t - 1)

        @pl.when(was_late)
        def _():
            late(m, 0)
            late(m, 1)

        @pl.when(t == slots - 1)
        def _():
            groups = rows // group // 2
            start = jnp.where(backward, groups, 0)
            flatten_rows(rows * n_row, tile, group, out_ref, start, groups, half_ref, 0)

        from_across(t)
        return now

    def take_cols(s):
        @pl.when(owns_cols)
        def _():
            cols[s] = full[s, pl.ds(aligned, span), :]

        @pl.when(jnp.logical_not(owns_cols))
        def _():
            pltpu.make_async_copy(cols.at[s], cols.at[s], col_recv.at[s]).wait()

    def columns(s):
        right = cols[s]
        if span != tile:
            right = jnp.where(offset == aligned, right[:tile], right[span - tile:])
        return right

    def add_product(sources, k):
        row = rows_of(sources[0], k)
        product = sum(
            lax.dot_general(
                full[s, row, :], columns(s), (((1,), (1,)), ((), ())), preferred_element_type=jnp.float32
            )
            for s in sources
        )
        for b in range(out_ref.shape[0]):
            width = min(128, tile - b * 128)
            out_ref[b, row, :width] += product[:, b * 128:b * 128 + width]

    def work(v, lane=None):
        e, m = cross_at(v - chunks)

        def one(n, _):
            sign = 1 - 2 * (n // 4)
            cross = lax.rem(n // 2, 2)
            distance = jnp.where(cross == 1, e, v // chunks)
            k = jnp.where(cross == 1, m, lax.rem(v, chunks))
            place = line + sign * distance
            good = jnp.logical_and(place >= 0, place < length)
            good = jnp.logical_and(good, distance >= n // 4)
            good = jnp.logical_and(good, jnp.logical_or(cross == 0, v >= chunks))
            if lane is not None:
                good = jnp.logical_and(good, lax.rem(n, 2) == lane)

            @pl.when(good)
            def _():
                s = index(place, lax.rem(side + cross, 2), lax.rem(n, 2))
                pl.when(k == 0)(lambda: take_cols(s))
                add_product([s], k)

            return 0

        lax.fori_loop(0, 8, one, 0)
        return 0

    def late(k, lane):
        add_product([index(near, 1 - side, lane)], k)

    def ready_own(k, _):
        s = index(line, side, 1 - core)
        arrived(s, k)
        to_peers(s, k)
        return 0

    lax.fori_loop(0, chunks, ready_own, 0)
    last = jnp.int32(slots - 1)
    if quick:
        lax.fori_loop(0, final, slot, 0)
        lax.fori_loop(final, slots, end_slot, done(jnp.int32(final - 1)))

        def finish(lane):
            @pl.when(jnp.logical_not(end))
            def _():
                work(last + chunks, lane)

            far = index(jnp.where(line == 0, length - 1, 0), 1 - side, lane)
            pl.when(end)(lambda: add_product([far, index(near, 1 - side, lane)], chunks - 1))

        finish(core)
        from_sibling(last)
        finish(1 - core)
    else:
        lax.fori_loop(0, slots, slot, 0)
        from_sibling(last)
        lax.fori_loop(done(last), slots + chunks, lambda v, _: work(v), 0)

    def sent(s, way, count):
        ref = full.at[s, pl.ds(0, count * size)]
        pltpu.make_async_copy(ref, ref, send.at[way, s]).wait()

    def some_sent(s, way, count):
        pl.when(count == chunks)(lambda: sent(s, way, chunks))
        if quick:
            pl.when(count == half)(lambda: sent(s, way, half))

    def drain(place, _):
        straight, cross = index(place, side, core), index(place, 1 - side, core)
        sent(straight, 3, chunks)
        sent(cross, 3, chunks)
        beside = jnp.logical_or(place == line + 1, place == line - 1)
        sign = place - line
        some_sent(straight, 2, jnp.where(beside, first_by_line(line, sign), chunks))
        pl.when(jnp.logical_and(has_up, place <= line))(lambda: sent(straight, 0, chunks))
        pl.when(jnp.logical_and(has_down, place >= line))(lambda: sent(straight, 1, chunks))

        @pl.when(place == line)
        def _():
            pl.when(has_up)(lambda: some_sent(cross, 0, chunks - first_by_line(line + 1, -1)))
            pl.when(has_down)(lambda: some_sent(cross, 1, chunks - first_by_line(line - 1, 1)))

        return 0

    lax.fori_loop(0, length, drain, 0)

    @pl.when(owns_cols)
    def _():
        for n in range(len(peers)):
            pltpu.make_async_copy(cols, cols, col_send.at[n]).wait()

    for n in range(len(peers)):
        pltpu.make_async_copy(sums.at[i], sums.at[i], sum_send.at[n]).wait()


def flatten_rows(members, tile, group, gram_ref, start, many, flat_ref, to_row):
    wide = group * tile // 128
    scale = jnp.float32(1.0 / (members - 1))
    first = start * group if isinstance(start, int) else pl.multiple_of(start * group, group)
    lane = lax.broadcasted_iota(jnp.int32, (many, 128), 1)
    for s in range(wide):
        value = None
        at = s * 128
        while at < (s + 1) * 128:
            r, c, to = at // tile, at % tile, at - s * 128
            count = min(tile - c, (s + 1) * 128 - at)
            shift = (to - c) % 128
            row = pl.ds(first + r, many, stride=group)
            here = gram_ref[c // 128, row, :]
            here = pltpu.roll(here, shift, 1) if shift else here
            if c % 128 + count > 128:
                then = gram_ref[c // 128 + 1, row, :]
                then = pltpu.roll(then, shift, 1) if shift else then
                here = jnp.where(lane < to + 128 - c % 128, here, then)
            value = here if value is None else jnp.where(lane < to, value, here)
            at += count
        flat_ref[pl.ds(to_row + s, many, stride=wide), :] = value * scale


def flatten(n_row, tile, group, gram_ref, *rest):
    members = gram_ref.shape[1] * n_row
    groups = gram_ref.shape[1] // group
    wide = group * tile // 128
    if len(rest) == 5:
        half_ref, flat_ref, buffer, sem, half_sem = rest
        groups //= 2
        backward = 2 * lax.axis_index("mrow") >= n_row
        start, done = jnp.where(backward, 0, groups), jnp.where(backward, groups, 0)
        half_copy = pltpu.make_async_copy(
            half_ref, flat_ref.at[pl.ds(pl.multiple_of(done * wide, 8), groups * wide)], half_sem
        )
        half_copy.start()
    else:
        flat_ref, buffer, sem = rest
        start, half_copy = 0, None
    for piece in range(0, groups, PIECE):
        many = min(PIECE, groups - piece)
        flatten_rows(members, tile, group, gram_ref, start + piece, many, buffer, piece * wide)
        target = (start + piece) * wide
        target = target if half_copy is None else pl.multiple_of(target, 8)
        pltpu.make_async_copy(
            buffer.at[pl.ds(piece * wide, many * wide)], flat_ref.at[pl.ds(target, many * wide)], sem
        ).start()
    pltpu.make_async_copy(buffer, flat_ref.at[pl.ds(0, groups * wide)], sem).wait()
    if half_copy is not None:
        half_copy.wait()


def local(n_row, n_col, snapshots, area_weight):
    rows, depth = snapshots.shape
    tile = rows * n_row // n_col
    units = rows // 16
    chunks = max(n for n in range(1, MAX_CHUNKS + 1) if units % n == 0)
    size = rows // chunks
    length = n_col // 4
    ends = [*range(4), *range(n_col - 4, n_col)]
    whole = size % tile == 0 and tile % 16 == 0 and chunks % 4 == 0
    quick = length > 2 and whole and all(trigger(n_row, n_col, chunks, size, tile, me) < chunks // 2 for me in ends)
    span = tile + tile % 16
    blocks = -(-tile // 128)
    group = 8
    while group * tile % 128:
        group *= 2
    flat_shape = (rows * tile // 128, 128)
    half_shape = (flat_shape[0] // 2, 128)
    quick = quick and rows % (16 * group) == 0 and half_shape[0] % 8 == 0
    shapes = [(blocks, rows, 128)] + [half_shape] * quick
    parts = pl.pallas_call(
        functools.partial(gather_gram, n_row, n_col, chunks, quick, tile, group),
        out_shape=[jax.ShapeDtypeStruct(shape, jnp.float32) for shape in shapes],
        in_specs=[pl.BlockSpec(memory_space=pltpu.VMEM)] * 2,
        out_specs=[pl.BlockSpec(memory_space=pltpu.VMEM)] * len(shapes),
        scratch_shapes=[
            pltpu.VMEM((n_col, rows, depth), jnp.bfloat16),
            pltpu.VMEM((n_col, span, depth), jnp.bfloat16),
            pltpu.VMEM((n_row, 8, depth), jnp.float32),
            pltpu.SemaphoreType.DMA((n_col, chunks)),
            pltpu.SemaphoreType.DMA((4, n_col)),
            pltpu.SemaphoreType.DMA((n_col,)),
            pltpu.SemaphoreType.DMA((max(n_row - 1, 1),)),
            pltpu.SemaphoreType.DMA((n_row,)),
            pltpu.SemaphoreType.DMA((max(n_row - 1, 1),)),
        ],
        compiler_params=pltpu.CompilerParams(
            collective_id=0, has_side_effects=True, vmem_limit_bytes=38 * 2**20
        ),
        name="gather_gram",
    )(snapshots, area_weight.reshape(1, depth))
    flat = pl.pallas_call(
        functools.partial(flatten, n_row, tile, group),
        out_shape=jax.ShapeDtypeStruct(flat_shape, jnp.float32),
        in_specs=[pl.BlockSpec(memory_space=pltpu.VMEM)] * len(shapes),
        out_specs=pl.BlockSpec(memory_space=pl.ANY),
        scratch_shapes=[
            pltpu.VMEM(half_shape if quick else flat_shape, jnp.float32),
            *[pltpu.SemaphoreType.DMA] * len(shapes),
        ],
        compiler_params=pltpu.CompilerParams(vmem_limit_bytes=16 * 2**20),
        name="flatten",
    )(*parts)
    return flat.reshape(1, 1, rows * tile)


def solution(mesh):
    placed = (P("mrow", "pcol"), P("pcol"))
    return jax.shard_map(
        functools.partial(local, mesh.shape["mrow"], mesh.shape["pcol"]),
        mesh=mesh, in_specs=placed, out_specs=P("mrow", "pcol", None), check_vma=False,
    )
```
